32 devices in a mesh: parts: 2 (over x), tiles: 16 (over z, y, core).
Axes of the slice: x: 2, y: 2, z: 4, core: 2. Of those that a mesh axis runs over, the one named last changes fastest.
Arguments:
- mask_params: float32 [4096, 1024], P(('parts', 'tiles')), parts along dimension 0, may hold values from -6 to 6
- target: int32 [4096, 1024], P(('parts', 'tiles')), parts along dimension 0, may hold values 0 or 1
- kernel_spectra: float32 [2, 16, 32, 128], replicated, may hold values from -0.0625 to 0.0625
- kernel_weights: float32 [16], replicated, may hold values from 0.05 to 1
Outputs:
- resist_image: float32 [4096, 1024], P(('parts', 'tiles')), parts along dimension 0
- mask_gradient: float32 [4096, 1024], P(('parts', 'tiles')), parts along dimension 0
The draws below stay inside these ranges and needn't reach their ends.
There are 2 independent parts, one for each index of `parts`. The reference program is written for one: setup_inputs(seed, part) draws one part's arguments, and reference() takes and returns one part's arrays. A program takes and returns all parts, laid end to end along the dimension named above; an argument that names none is the same for every part. Nothing has to cross between parts.
All inputs are finite; a program needn't handle non-finite values. No bound on the sum of `target` on one device may be relied on, other than what follows from the above.
Results may differ from the reference program's by a relative error of at most 0.0003.
Values sent between devices are 32-bit elements; how exact they have to be, the bound alone decides.
No kernel may reach another device: no remote copies, remote signals or barrier semaphores. Data moves between devices by JAX's collectives and lax.ppermute only.
A program may use at most 64 MiB of HBM per device.

```python
import math
import jax
import jax.numpy as jnp
from jax import lax

ROWS_DEV = 128
COLS = 1024
MARGIN = 64
KERNELS = 16
WINDOW = 256
FREQ_ROWS = 32
FREQ_COLS = 128
ROWS = 2048
N_TILES = 16


def touch_ends(result, rng, least, largest):
    index_at = [jax.random.randint(jax.random.fold_in(rng, axis), (), 0, length) for axis, length in enumerate(result.shape)]
    longest = result.shape.index(max(result.shape))
    beside = index_at[:longest] + [(index_at[longest] + 1) % result.shape[longest]] + index_at[longest + 1:]
    return result.at[tuple(index_at)].set(least).at[tuple(beside)].set(largest)


def block_scale(key, extent, cuts, least, high):
    def one(axis_at, shards_of):
        draws = jax.random.uniform(jax.random.fold_in(jax.random.fold_in(key, 6), axis_at), (shards_of,), jnp.float32, least / len(cuts), high / len(cuts))
        return jnp.repeat(jnp.exp(draws), extent[axis_at] // shards_of).reshape((-1,) + (1,) * (len(extent) - axis_at - 1))

    level = one(*cuts[0])
    for cut in cuts[1:]:
        level = level * one(*cut)
    return level


def scatter_about(key, dims, spread, limit, shards=(), held_as=jnp.bfloat16):
    drawn = spread * jax.random.normal(key, dims, jnp.float32)
    if shards:
        drawn = drawn * block_scale(key, dims, shards, -0.22, 0.18)
    return jnp.clip(drawn, -limit, limit).astype(held_as)


def setup_inputs(seed: int = 0, part: int = 0) -> dict:
    key_of = jax.random.split(jax.random.key(seed), 5)
    part_keys = jax.random.split(jax.random.fold_in(key_of[4], part), 5)
    return {
        "mask_params": scatter_about(part_keys[0], (ROWS, COLS), 1.0, 6.0, ((0, 16),), jnp.float32),
        "target": touch_ends((jax.random.randint(part_keys[1], (ROWS, COLS), 0, 2) < 1).astype(jnp.int32), jax.random.fold_in(part_keys[1], 1), 0, 1),
        "kernel_spectra": scatter_about(key_of[2], (2, KERNELS, FREQ_ROWS, FREQ_COLS), (2 * FREQ_ROWS * FREQ_COLS) ** -0.5, 0.0625, (), jnp.float32),
        "kernel_weights": jnp.clip(jnp.exp(jax.random.uniform(key_of[3], (KERNELS,), jnp.float32, math.log(0.05), math.log(1.0))), 0.05, 1.0),
    }


STEEPNESS = 8.0
THRESHOLD = 0.35
HIGHEST = lax.Precision.HIGHEST

def matmul(left, right):
    return jnp.dot(left, right, precision=HIGHEST, preferred_element_type=jnp.float32)

def phase_table(frequencies, positions, length):
    cycles = jnp.remainder(frequencies[:, None] * positions[None, :], length).astype(jnp.float32)
    angles = cycles * (2.0 * math.pi / length)
    return (jnp.cos(angles), jnp.sin(angles))

def make_tables(strip_rows, margin, columns, freq_rows, freq_cols):
    window = strip_rows + 2 * margin
    col_freq = jnp.arange(freq_cols, dtype=jnp.int32) - freq_cols // 2
    row_freq = jnp.arange(freq_rows, dtype=jnp.int32) - freq_rows // 2
    col_cos, col_sin = phase_table(col_freq, jnp.arange(columns, dtype=jnp.int32), columns)
    row_cos, row_sin = phase_table(row_freq, jnp.arange(window, dtype=jnp.int32), window)
    factor = 1.0 / math.sqrt(window * columns)
    forward_cols = jnp.concatenate([col_cos.T, -col_sin.T], axis=1) * factor
    row_stack = jnp.concatenate([row_cos, row_sin], axis=0)
    own_rows = row_stack[:, margin:margin + strip_rows].T
    inverse_cols = jnp.concatenate([jnp.concatenate([col_cos, col_sin], axis=1), jnp.concatenate([-col_sin, col_cos], axis=1)], axis=0)
    return (forward_cols, row_stack, own_rows, inverse_cols)

def kernel_fields(window_spec, kernel_spectra, own_rows):
    half_rows = window_spec.shape[0] // 2
    half_cols = window_spec.shape[1] // 2
    spec_real = window_spec[:half_rows, :half_cols] + window_spec[half_rows:, half_cols:]
    spec_imag = window_spec[:half_rows, half_cols:] - window_spec[half_rows:, :half_cols]
    kern_real = kernel_spectra[0]
    kern_imag = kernel_spectra[1]
    prod_real = kern_real * spec_real - kern_imag * spec_imag
    prod_imag = kern_real * spec_imag + kern_imag * spec_real
    blocked = jnp.concatenate([jnp.concatenate([prod_real, prod_imag], axis=2), jnp.concatenate([-prod_imag, prod_real], axis=2)], axis=1)
    return jnp.einsum('pr,krc->kpc', own_rows, blocked, precision=HIGHEST)

def window_adjoint(inner_grad, kernel_spectra, own_rows):
    half_rows = own_rows.shape[1] // 2
    half_cols = inner_grad.shape[2] // 2
    spec_grad = jnp.einsum('pr,kpc->krc', own_rows, inner_grad, precision=HIGHEST)
    grad_real = spec_grad[:, :half_rows, :half_cols] + spec_grad[:, half_rows:, half_cols:]
    grad_imag = spec_grad[:, :half_rows, half_cols:] - spec_grad[:, half_rows:, :half_cols]
    kern_real = kernel_spectra[0]
    kern_imag = kernel_spectra[1]
    win_real = lax.optimization_barrier(jnp.sum(grad_real * kern_real + grad_imag * kern_imag, axis=0))
    win_imag = lax.optimization_barrier(jnp.sum(grad_imag * kern_real - grad_real * kern_imag, axis=0))
    return jnp.concatenate([jnp.concatenate([win_real, win_imag], axis=1), jnp.concatenate([-win_imag, win_real], axis=1)], axis=0)

def strip_step(window_rows, target_rows, kernel_spectra, kernel_weights, tables):
    forward_cols, row_stack, own_rows, inverse_cols = tables
    columns = window_rows.shape[1]
    window_spec = matmul(row_stack, matmul(window_rows, forward_cols))
    inner = kernel_fields(window_spec, kernel_spectra, own_rows)
    fields = jnp.einsum('kpc,cw->kpw', inner, inverse_cols, precision=HIGHEST)
    shares = kernel_weights / jnp.sum(kernel_weights)
    powers = fields[:, :, :columns] ** 2 + fields[:, :, columns:] ** 2
    intensity = jnp.einsum('k,kpw->pw', shares, powers, precision=HIGHEST)
    resist = jax.nn.sigmoid(STEEPNESS * (intensity - THRESHOLD))
    slopes = 2.0 * (resist - target_rows.astype(jnp.float32)) * STEEPNESS * resist * (1.0 - resist)
    doubled = jnp.concatenate([slopes, slopes], axis=1)
    field_grad = (2.0 * shares)[:, None, None] * doubled[None] * fields
    inner_grad = jnp.einsum('kpw,cw->kpc', field_grad, inverse_cols, precision=HIGHEST)
    window_grad = window_adjoint(inner_grad, kernel_spectra, own_rows)
    back_rows = matmul(matmul(row_stack.T, window_grad), forward_cols.T)
    return (resist, back_rows)

def reference(mask_params, target, kernel_spectra, kernel_weights):
    transmit = jnp.tanh(mask_params)
    tables = make_tables(ROWS_DEV, MARGIN, COLS, FREQ_ROWS, FREQ_COLS)
    padded = jnp.concatenate([transmit[ROWS - MARGIN:], transmit, transmit[:MARGIN]], axis=0)

    def per_strip(running, strip_index):
        offset = (strip_index * ROWS_DEV).astype(jnp.int32)
        window_rows = lax.dynamic_slice_in_dim(padded, offset, WINDOW, 0)
        target_rows = lax.dynamic_slice_in_dim(target, offset, ROWS_DEV, 0)
        resist, back_rows = strip_step(window_rows, target_rows, kernel_spectra, kernel_weights, tables)
        before = lax.dynamic_slice_in_dim(running, offset, WINDOW, 0)
        running = lax.dynamic_update_slice_in_dim(running, before + back_rows, offset, 0)
        return (running, resist)
    start = jnp.zeros((ROWS + 2 * MARGIN, COLS), jnp.float32)
    totals, resist = lax.scan(per_strip, start, jnp.arange(N_TILES, dtype=jnp.int32))
    mask_grad = totals[MARGIN:MARGIN + ROWS]
    mask_grad = mask_grad.at[:MARGIN].add(totals[ROWS + MARGIN:])
    mask_grad = mask_grad.at[ROWS - MARGIN:].add(totals[:MARGIN])
    gradient = mask_grad * (1.0 - transmit * transmit)
    return (resist.reshape(ROWS, COLS), gradient)
```

```python
import functools
import math

import jax
import jax.numpy as jnp
import numpy as np
from jax import lax
from jax.experimental import pallas as pl
from jax.experimental.pallas import tpu as pltpu
from jax.sharding import PartitionSpec as P

MARGIN = 64

STEEPNESS = 8.0
THRESHOLD = 0.35

BF16 = jnp.bfloat16
F32 = jnp.float32


def split_table(table):
    table = np.asarray(table, np.float32)
    high = table.astype(BF16)
    low = (table - high.astype(np.float32)).astype(BF16)
    return high, low


def stack_left(table):
    high, low = split_table(table)
    return np.concatenate([high, high, low], axis=1)


def angles(frequencies, positions, period):
    cycles = np.remainder(frequencies[:, None] * positions[None, :], period)
    return cycles * (2.0 * math.pi / period)


def interpolation(fine, coarse, bound, period):
    count = len(coarse)
    distance = fine[:, None] - coarse[None, :]
    total = np.ones_like(distance, dtype=np.float64)
    for frequency in range(1, bound):
        total += 2.0 * np.cos(np.remainder(frequency * distance, period) * (2.0 * math.pi / period))
    return total / count


def make_tables(strip_rows, margin, columns, freq_rows, freq_cols):
    window = strip_rows + 2 * margin
    row_freq = np.arange(freq_rows, dtype=np.float64) - freq_rows // 2
    col_freq = np.arange(freq_cols, dtype=np.float64) - freq_cols // 2
    rows_c, cols_c = 2 * freq_rows, 2 * freq_cols
    own = np.arange(margin, margin + strip_rows, dtype=np.float64)
    wide = np.arange(columns, dtype=np.float64)
    samples_r = np.arange(rows_c, dtype=np.float64) * (window / rows_c)
    samples_c = np.arange(cols_c, dtype=np.float64) * (columns / cols_c)
    factor = 1.0 / math.sqrt(window * columns)
    col_angle = angles(col_freq, wide, columns)
    forward = np.concatenate([np.cos(col_angle).T, -np.sin(col_angle).T], axis=1) * factor
    row_angle = angles(row_freq, own, window)
    cos_r, sin_r = np.cos(row_angle), np.sin(row_angle)
    half = strip_rows // 2
    none = np.zeros((freq_rows, half))
    first = np.concatenate([cos_r[:, :half], none, sin_r[:, :half], none], axis=1)
    second = np.concatenate([none, cos_r[:, half:], none, sin_r[:, half:]], axis=1)
    project = np.concatenate([first, second], axis=0)
    back_rows = np.concatenate([cos_r, sin_r], axis=0).T
    coarse_r = angles(row_freq, samples_r, window)
    field_rows = np.concatenate([np.cos(coarse_r), np.sin(coarse_r)], axis=0).T
    coarse_c = angles(col_freq, samples_c, columns)
    cos_c, sin_c = np.cos(coarse_c), np.sin(coarse_c)
    field_cols = np.concatenate(
        [np.concatenate([cos_c, sin_c], axis=1), np.concatenate([-sin_c, cos_c], axis=1)], axis=0
    )
    widen_rows = interpolation(own, samples_r, freq_rows, window)
    widen_cols = interpolation(wide, samples_c, freq_cols, columns).T
    return {
        "forward": split_table(forward),
        "project": split_table(project),
        "back_rows": stack_left(back_rows),
        "field_rows": stack_left(field_rows),
        "field_rows_t": stack_left(field_rows.T),
        "field_cols": split_table(field_cols),
        "widen_rows": stack_left(widen_rows),
        "widen_rows_t": stack_left(widen_rows.T),
        "widen_cols": split_table(widen_cols),
    }


def split(value):
    high = value.astype(BF16)
    return high, (value - high.astype(F32)).astype(BF16)


def stack_right(value):
    high, low = split(value)
    return jnp.concatenate([high, low, high], axis=0)


def dot(left, right):
    return jnp.dot(left, right, preferred_element_type=F32)


def dot_t(left, right):
    return lax.dot_general(left, right, (((1,), (1,)), ((), ())), preferred_element_type=F32)


def dot3(left, right):
    (lh, ll), (rh, rl) = left, right
    return dot(lh, rh) + dot(lh, rl) + dot(ll, rh)


def dot3_t(left, right):
    (lh, ll), (rh, rl) = left, right
    return dot_t(lh, rh) + dot_t(lh, rl) + dot_t(ll, rh)


def turn(pair, sign):
    half = pair.shape[1] // 2
    real, imag = pair[:, :half], pair[:, half:]
    if sign > 0:
        turned = jnp.concatenate([-imag, real], axis=1)
    else:
        turned = jnp.concatenate([imag, -real], axis=1)
    return jnp.concatenate([pair, turned], axis=0)


def alternate(shape):
    row = lax.broadcasted_iota(jnp.int32, shape, 0)
    return jnp.where(row % 2 == 0, 1.0, -1.0).astype(F32)


def project_kernel(mask, fwd_h, fwd_l, proj_h, proj_l, low_out, high_out, slope_out):
    transmit = jnp.tanh(mask[...])
    slope_out[...] = 1.0 - transmit * transmit
    spectra = dot3(split(transmit), (fwd_h[...], fwd_l[...]))
    parts = dot3((proj_h[...], proj_l[...]), split(turn(spectra, -1)))
    freq_rows = low_out.shape[0]
    low_out[...] = parts[:freq_rows]
    high_out[...] = parts[freq_rows:]


def image_kernel(
    low, high, before, after, spectra, target, rows_f, rows_t, cols_h, cols_l,
    wide_r, wide_rt, wide_h, wide_l, resist_out, grad_out, fields
):
    kernels, freq_rows, freq_cols = spectra.shape[1:]
    rows_c, cols_c = rows_f.shape[0], 2 * freq_cols
    sign = alternate(low.shape)
    window = low[...] + high[...] + sign * (before[...] + after[...])
    win_re, win_im = window[:, :freq_cols], window[:, freq_cols:]
    group = 4
    total = jnp.zeros((rows_c, cols_c), F32)
    for start in range(0, kernels, group):
        inners = []
        for k in range(start, start + group):
            kern_re, kern_im = spectra[0, k], spectra[1, k]
            prod = jnp.concatenate(
                [kern_re * win_re - kern_im * win_im, kern_re * win_im + kern_im * win_re], axis=1
            )
            inners.append(dot(rows_f[...], stack_right(turn(prod, 1))))
        inner = jnp.concatenate(inners, axis=0)
        field = dot3(split(inner), (cols_h[...], cols_l[...]))
        fields[pl.ds(start * rows_c, group * rows_c), :] = field
        power = field[:, :cols_c] ** 2 + field[:, cols_c:] ** 2
        for j in range(group):
            total = total + power[j * rows_c : (j + 1) * rows_c]
    tall = dot(wide_r[...], stack_right(total))
    intensity = dot3(split(tall), (wide_h[...], wide_l[...]))
    resist = jax.nn.sigmoid(STEEPNESS * (intensity - THRESHOLD))
    resist_out[...] = resist
    slopes = (4.0 * STEEPNESS) * (resist - target[...].astype(F32)) * resist * (1.0 - resist)
    narrow = dot3_t(split(slopes), (wide_h[...], wide_l[...]))
    weight = dot(wide_rt[...], stack_right(narrow))
    weight = jnp.concatenate([weight, weight], axis=1)
    grad_re = jnp.zeros((freq_rows, freq_cols), F32)
    grad_im = jnp.zeros((freq_rows, freq_cols), F32)
    for start in range(0, kernels, group):
        scaled = jnp.concatenate(
            [weight * fields[pl.ds(k * rows_c, rows_c), :] for k in range(start, start + group)],
            axis=0,
        )
        inner = dot3_t(split(scaled), (cols_h[...], cols_l[...]))
        for j in range(group):
            k = start + j
            spec = dot(rows_t[...], stack_right(inner[j * rows_c : (j + 1) * rows_c]))
            real = spec[:freq_rows, :freq_cols] + spec[freq_rows:, freq_cols:]
            imag = spec[:freq_rows, freq_cols:] - spec[freq_rows:, :freq_cols]
            kern_re, kern_im = spectra[0, k], spectra[1, k]
            grad_re = grad_re + real * kern_re + imag * kern_im
            grad_im = grad_im + imag * kern_re - real * kern_im
    grad_out[...] = jnp.concatenate([grad_re, grad_im], axis=1)


def gradient_kernel(own, before, after, slope, rows_b, fwd_h, fwd_l, out):
    half = out.shape[0] // 2
    sign = alternate(own.shape)
    low = stack_right(turn(own[...] + sign * before[...], 1))
    high = stack_right(turn(own[...] + sign * after[...], 1))
    merged = jnp.concatenate([dot(rows_b[:half], low), dot(rows_b[half:], high)], axis=0)
    out[...] = slope[...] * dot3_t(split(merged), (fwd_h[...], fwd_l[...]))


def call(kernel, outs, args, flops, scratch=(), limit=32 << 20):
    vmem = pl.BlockSpec(memory_space=pltpu.VMEM)
    shapes = [jax.ShapeDtypeStruct(shape, F32) for shape in outs]
    moved = sum(math.prod(a.shape) * a.dtype.itemsize for a in args)
    moved += sum(4 * math.prod(shape) for shape in outs)
    return pl.pallas_call(
        kernel,
        out_shape=shapes,
        in_specs=[vmem] * len(args),
        out_specs=[vmem] * len(outs),
        scratch_shapes=scratch,
        compiler_params=pltpu.CompilerParams(vmem_limit_bytes=limit),
        cost_estimate=pl.CostEstimate(flops=flops, bytes_accessed=moved, transcendentals=0),
    )(*args)


def shards(mask_params, target, kernel_spectra, kernel_weights):
    strip_rows, columns = mask_params.shape
    kernels, freq_rows, freq_cols = kernel_spectra.shape[1:]
    assert 2 * MARGIN == strip_rows
    tables = jax.tree.map(
        jnp.asarray, make_tables(strip_rows, MARGIN, columns, freq_rows, freq_cols)
    )
    count = lax.axis_size("tiles")
    forward = [(i, (i + 1) % count) for i in range(count)]
    backward = [(j, i) for i, j in forward]
    pair = (freq_rows, 2 * freq_cols)
    area = strip_rows * columns
    low, high, slope = call(
        project_kernel,
        [pair, pair, (strip_rows, columns)],
        [mask_params, *tables["forward"], *tables["project"]],
        flops=6 * area * 2 * freq_cols,
    )
    before = lax.ppermute(high, "tiles", forward)
    after = lax.ppermute(low, "tiles", backward)
    shares = jnp.sqrt(kernel_weights / jnp.sum(kernel_weights))
    spectra = kernel_spectra * shares[None, :, None, None]
    rows_c, cols_c = 2 * freq_rows, 2 * freq_cols
    resist, grad = call(
        image_kernel,
        [(strip_rows, columns), pair],
        [
            low, high, before, after, spectra, target,
            tables["field_rows"], tables["field_rows_t"], *tables["field_cols"],
            tables["widen_rows"], tables["widen_rows_t"], *tables["widen_cols"],
        ],
        flops=24 * kernels * rows_c * cols_c * cols_c,
        scratch=[pltpu.VMEM((kernels * rows_c, 2 * cols_c), F32)],
    )
    grad_before = lax.ppermute(grad, "tiles", forward)
    grad_after = lax.ppermute(grad, "tiles", backward)
    (gradient,) = call(
        gradient_kernel,
        [(strip_rows, columns)],
        [grad, grad_before, grad_after, slope, tables["back_rows"], *tables["forward"]],
        flops=6 * area * 2 * freq_cols,
    )
    return (resist, gradient)


def solution(mesh):
    in_specs = (P(("parts", "tiles"), None), P(("parts", "tiles"), None), P(), P())
    out_specs = (P(("parts", "tiles"), None), P(("parts", "tiles"), None))
    return jax.shard_map(shards, mesh=mesh, in_specs=in_specs, out_specs=out_specs, check_vma=False)
```

```python
import math

import jax
import jax.numpy as jnp
import numpy as np
from jax import lax
from jax.experimental import pallas as pl
from jax.experimental.pallas import tpu as pltpu
from jax.sharding import PartitionSpec as P

MARGIN = 64

STEEPNESS = 8.0
THRESHOLD = 0.35

BF16 = jnp.bfloat16
F32 = jnp.float32
CHUNKS = 4


def split_table(table):
    table = np.asarray(table, np.float32)
    high = table.astype(BF16)
    low = (table - high.astype(np.float32)).astype(BF16)
    return high, low


def stack_left(table):
    high, low = split_table(table)
    return np.concatenate([high, high, low], axis=1)


def angles(frequencies, positions, period):
    cycles = np.remainder(frequencies[:, None] * positions[None, :], period)
    return cycles * (2.0 * math.pi / period)


def interpolation(fine, coarse, bound, period):
    count = len(coarse)
    distance = fine[:, None] - coarse[None, :]
    total = np.ones_like(distance, dtype=np.float64)
    for frequency in range(1, bound):
        total += 2.0 * np.cos(np.remainder(frequency * distance, period) * (2.0 * math.pi / period))
    return total / count


def make_tables(strip_rows, margin, columns, freq_rows, freq_cols):
    window = strip_rows + 2 * margin
    row_freq = np.arange(freq_rows, dtype=np.float64) - freq_rows // 2
    col_freq = np.arange(freq_cols, dtype=np.float64) - freq_cols // 2
    rows_c, cols_c = 2 * freq_rows, 2 * freq_cols
    own = np.arange(margin, margin + strip_rows, dtype=np.float64)
    wide = np.arange(columns, dtype=np.float64)
    samples_r = np.arange(rows_c, dtype=np.float64) * (window / rows_c)
    samples_c = np.arange(cols_c, dtype=np.float64) * (columns / cols_c)
    factor = 1.0 / math.sqrt(window * columns)
    col_angle = angles(col_freq, wide, columns)
    forward = np.concatenate([np.cos(col_angle).T, -np.sin(col_angle).T], axis=1) * factor
    row_angle = angles(row_freq, own, window)
    cos_r, sin_r = np.cos(row_angle), np.sin(row_angle)
    half = strip_rows // 2
    none = np.zeros((freq_rows, half))
    first = np.concatenate([cos_r[:, :half], none, sin_r[:, :half], none], axis=1)
    second = np.concatenate([none, cos_r[:, half:], none, sin_r[:, half:]], axis=1)
    project = np.concatenate([first, second], axis=0)
    back_rows = np.concatenate([cos_r, sin_r], axis=0).T
    coarse_r = angles(row_freq, samples_r, window)
    field_rows = np.concatenate([np.cos(coarse_r), np.sin(coarse_r)], axis=0).T
    coarse_c = angles(col_freq, samples_c, columns)
    cos_c, sin_c = np.cos(coarse_c), np.sin(coarse_c)
    field_cols = np.concatenate(
        [np.concatenate([cos_c, sin_c], axis=1), np.concatenate([-sin_c, cos_c], axis=1)], axis=0
    )
    widen_rows = interpolation(own, samples_r, freq_rows, window)
    widen_cols = interpolation(wide, samples_c, freq_cols, columns).T
    return {
        "forward": split_table(forward),
        "project": split_table(project),
        "back_rows": stack_left(back_rows),
        "field_rows": stack_left(field_rows),
        "field_rows_t": stack_left(field_rows.T),
        "field_cols": split_table(field_cols),
        "widen_rows": stack_left(widen_rows),
        "widen_rows_t": stack_left(widen_rows.T),
        "widen_cols": split_table(widen_cols),
    }


def split(value):
    high = value.astype(BF16)
    return high, (value - high.astype(F32)).astype(BF16)


def stack_right(value):
    high, low = split(value)
    return jnp.concatenate([high, low, high], axis=0)


def dot(left, right):
    return jnp.dot(left, right, preferred_element_type=F32)


def dot_t(left, right):
    return lax.dot_general(left, right, (((1,), (1,)), ((), ())), preferred_element_type=F32)


def dot3(left, right):
    (lh, ll), (rh, rl) = left, right
    return dot(lh, rh) + dot(lh, rl) + dot(ll, rh)


def dot3_t(left, right):
    (lh, ll), (rh, rl) = left, right
    return dot_t(lh, rh) + dot_t(lh, rl) + dot_t(ll, rh)


def turn(pair, sign):
    half = pair.shape[1] // 2
    real, imag = pair[:, :half], pair[:, half:]
    if sign > 0:
        turned = jnp.concatenate([-imag, real], axis=1)
    else:
        turned = jnp.concatenate([imag, -real], axis=1)
    return jnp.concatenate([pair, turned], axis=0)


def alternate(shape):
    row = lax.broadcasted_iota(jnp.int32, shape, 0)
    return jnp.where(row % 2 == 0, 1.0, -1.0).astype(F32)


def is_odd():
    return lax.axis_index("tiles") % 2 == 1


def column_chunks(ref, chunks):
    width = ref.shape[1] // chunks
    return [pl.ds(i * width, width) for i in range(chunks)]


def project_kernel(
    mask_hbm, fwd_h_hbm, fwd_l_hbm, proj_h_hbm, proj_l_hbm, far_out, near_out, sum_out, slope_out,
    mask, fwd_h, fwd_l, proj_h, proj_l, sems
):
    chunks = column_chunks(mask, CHUNKS)
    copies = []
    for i, cols in enumerate(chunks):
        copies.append([
            pltpu.make_async_copy(mask_hbm.at[:, cols], mask.at[:, cols], sems.at[0, i]),
            pltpu.make_async_copy(fwd_h_hbm.at[cols, :], fwd_h.at[cols, :], sems.at[1, i]),
            pltpu.make_async_copy(fwd_l_hbm.at[cols, :], fwd_l.at[cols, :], sems.at[2, i]),
        ])
    last = [
        pltpu.make_async_copy(proj_h_hbm, proj_h, sems.at[3, 0]),
        pltpu.make_async_copy(proj_l_hbm, proj_l, sems.at[3, 1]),
    ]
    for group in copies:
        for copy in group:
            copy.start()
    for copy in last:
        copy.start()
    spectra = None
    for group, cols in zip(copies, chunks):
        group[0].wait()
        transmit = jnp.tanh(mask[:, cols])
        slope_out[:, cols] = 1.0 - transmit * transmit
        pieces = split(transmit)
        group[1].wait()
        group[2].wait()
        term = dot3(pieces, (fwd_h[cols, :], fwd_l[cols, :]))
        spectra = term if spectra is None else spectra + term
    for copy in last:
        copy.wait()
    parts = dot3((proj_h[...], proj_l[...]), split(turn(spectra, -1)))
    freq_rows = far_out.shape[0]
    low, high = parts[:freq_rows], parts[freq_rows:]
    odd = is_odd()
    far_out[...] = jnp.where(odd, high, low)
    near_out[...] = jnp.where(odd, low, high)
    sum_out[...] = low + high


def image_kernel(
    own, far, near, spectra, target, rows_f, rows_t, cols_h, cols_l,
    wide_r, wide_rt, wide_h, wide_l, resist_hbm, grad_out, fields, resist_out, sem
):
    kernels, freq_rows, freq_cols = spectra.shape[1:]
    rows_c, cols_c = rows_f.shape[0], 2 * freq_cols
    sign = alternate(own.shape)
    window = own[...] + sign * (far[...] + near[...])
    win_re, win_im = window[:, :freq_cols], window[:, freq_cols:]
    group = 4
    total = jnp.zeros((rows_c, cols_c), F32)
    for start in range(0, kernels, group):
        inners = []
        for k in range(start, start + group):
            kern_re, kern_im = spectra[0, k], spectra[1, k]
            prod = jnp.concatenate(
                [kern_re * win_re - kern_im * win_im, kern_re * win_im + kern_im * win_re], axis=1
            )
            inners.append(dot(rows_f[...], stack_right(turn(prod, 1))))
        inner = jnp.concatenate(inners, axis=0)
        field = dot3(split(inner), (cols_h[...], cols_l[...]))
        fields[pl.ds(start * rows_c, group * rows_c), :] = field
        power = field[:, :cols_c] ** 2 + field[:, cols_c:] ** 2
        for j in range(group):
            total = total + power[j * rows_c : (j + 1) * rows_c]
    tall = dot(wide_r[...], stack_right(total))
    intensity = dot3(split(tall), (wide_h[...], wide_l[...]))
    resist = jax.nn.sigmoid(STEEPNESS * (intensity - THRESHOLD))
    resist_out[...] = resist
    sent = pltpu.make_async_copy(resist_out, resist_hbm, sem)
    sent.start()
    slopes = (4.0 * STEEPNESS) * (resist - target[...].astype(F32)) * resist * (1.0 - resist)
    narrow = dot3_t(split(slopes), (wide_h[...], wide_l[...]))
    weight = dot(wide_rt[...], stack_right(narrow))
    weight = jnp.concatenate([weight, weight], axis=1)
    grad_re = jnp.zeros((freq_rows, freq_cols), F32)
    grad_im = jnp.zeros((freq_rows, freq_cols), F32)
    for start in range(0, kernels, group):
        scaled = jnp.concatenate(
            [weight * fields[pl.ds(k * rows_c, rows_c), :] for k in range(start, start + group)],
            axis=0,
        )
        inner = dot3_t(split(scaled), (cols_h[...], cols_l[...]))
        for j in range(group):
            k = start + j
            spec = dot(rows_t[...], stack_right(inner[j * rows_c : (j + 1) * rows_c]))
            real = spec[:freq_rows, :freq_cols] + spec[freq_rows:, freq_cols:]
            imag = spec[:freq_rows, freq_cols:] - spec[freq_rows:, :freq_cols]
            kern_re, kern_im = spectra[0, k], spectra[1, k]
            grad_re = grad_re + real * kern_re + imag * kern_im
            grad_im = grad_im + imag * kern_re - real * kern_im
    grad_out[...] = jnp.concatenate([grad_re, grad_im], axis=1)
    sent.wait()


def gradient_kernel(own, far, near, slope, rows_b, fwd_h, fwd_l, out_hbm, out, sems):
    half = out.shape[0] // 2
    sign = alternate(own.shape)
    odd = is_odd()
    before = jnp.where(odd, near[...], far[...])
    after = jnp.where(odd, far[...], near[...])
    low = stack_right(turn(own[...] + sign * before, 1))
    high = stack_right(turn(own[...] + sign * after, 1))
    merged = jnp.concatenate([dot(rows_b[:half], low), dot(rows_b[half:], high)], axis=0)
    merged = split(merged)
    sent = []
    for i, cols in enumerate(column_chunks(out, CHUNKS)):
        out[:, cols] = slope[:, cols] * dot3_t(merged, (fwd_h[cols, :], fwd_l[cols, :]))
        sent.append(pltpu.make_async_copy(out.at[:, cols], out_hbm.at[:, cols], sems.at[i]))
        sent[-1].start()
    for copy in sent:
        copy.wait()


VMEM = pl.BlockSpec(memory_space=pltpu.VMEM)
HBM = pl.BlockSpec(memory_space=pltpu.HBM)


def call(kernel, outs, args, flops, scratch, out_specs, in_specs=None, limit=32 << 20):
    shapes = [jax.ShapeDtypeStruct(shape, F32) for shape in outs]
    moved = sum(math.prod(a.shape) * a.dtype.itemsize for a in args)
    moved += sum(4 * math.prod(shape) for shape in outs)
    return pl.pallas_call(
        kernel,
        out_shape=shapes,
        in_specs=in_specs or [VMEM] * len(args),
        out_specs=out_specs,
        scratch_shapes=scratch,
        compiler_params=pltpu.CompilerParams(vmem_limit_bytes=limit),
        cost_estimate=pl.CostEstimate(flops=flops, bytes_accessed=moved, transcendentals=0),
    )(*args)


def shards(mask_params, target, kernel_spectra, kernel_weights):
    strip_rows, columns = mask_params.shape
    kernels, freq_rows, freq_cols = kernel_spectra.shape[1:]
    tables = jax.tree.map(
        jnp.asarray, make_tables(strip_rows, MARGIN, columns, freq_rows, freq_cols)
    )
    count = lax.axis_size("tiles")
    assert 2 * MARGIN == strip_rows and count % 2 == 0
    near_pairs = [(i, i ^ 1) for i in range(count)]
    far_pairs = [(i, (i + 1 if i % 2 else i - 1) % count) for i in range(count)]
    pair = (freq_rows, 2 * freq_cols)
    area = strip_rows * columns
    args = [mask_params, *tables["forward"], *tables["project"]]
    args = [pltpu.with_memory_space_constraint(a, pltpu.HBM) for a in args]
    send_far, send_near, own, slope = call(
        project_kernel,
        [pair, pair, pair, (strip_rows, columns)],
        args,
        flops=6 * area * 2 * freq_cols,
        scratch=[pltpu.VMEM(a.shape, a.dtype) for a in args]
        + [pltpu.SemaphoreType.DMA((4, CHUNKS))],
        in_specs=[HBM] * len(args),
        out_specs=[VMEM] * 4,
    )
    far = lax.ppermute(send_far, "tiles", far_pairs)
    near = lax.ppermute(send_near, "tiles", near_pairs)
    shares = jnp.sqrt(kernel_weights / jnp.sum(kernel_weights))
    spectra = kernel_spectra * shares[None, :, None, None]
    rows_c, cols_c = 2 * freq_rows, 2 * freq_cols
    resist, grad = call(
        image_kernel,
        [(strip_rows, columns), pair],
        [
            own, far, near, spectra, target,
            tables["field_rows"], tables["field_rows_t"], *tables["field_cols"],
            tables["widen_rows"], tables["widen_rows_t"], *tables["widen_cols"],
        ],
        flops=24 * kernels * rows_c * cols_c * cols_c,
        scratch=[
            pltpu.VMEM((kernels * rows_c, 2 * cols_c), F32),
            pltpu.VMEM((strip_rows, columns), F32),
            pltpu.SemaphoreType.DMA,
        ],
        out_specs=[HBM, VMEM],
    )
    grad_far = lax.ppermute(grad, "tiles", far_pairs)
    grad_near = lax.ppermute(grad, "tiles", near_pairs)
    (gradient,) = call(
        gradient_kernel,
        [(strip_rows, columns)],
        [grad, grad_far, grad_near, slope, tables["back_rows"], *tables["forward"]],
        flops=6 * area * 2 * freq_cols,
        scratch=[pltpu.VMEM((strip_rows, columns), F32), pltpu.SemaphoreType.DMA((CHUNKS,))],
        out_specs=[HBM],
    )
    return (resist, gradient)


def solution(mesh):
    in_specs = (P(("parts", "tiles"), None), P(("parts", "tiles"), None), P(), P())
    out_specs = (P(("parts", "tiles"), None), P(("parts", "tiles"), None))
    return jax.shard_map(shards, mesh=mesh, in_specs=in_specs, out_specs=out_specs, check_vma=False)
```

```python
import math

import jax
import jax.numpy as jnp
import numpy as np
from jax import lax
from jax.experimental import pallas as pl
from jax.experimental.pallas import tpu as pltpu
from jax.sharding import PartitionSpec as P


MARGIN = 64

STEEPNESS = 8.0
THRESHOLD = 0.35

BF16 = jnp.bfloat16
F32 = jnp.float32
QUARTERS = 4
GROUP = 8
LIMIT = 32 << 20


def split_table(table):
    table = np.asarray(table, np.float32)
    high = table.astype(BF16)
    low = (table - high.astype(np.float32)).astype(BF16)
    return high, low


def stack_left(table):
    high, low = split_table(table)
    return np.concatenate([high, high, low], axis=1)


def angles(frequencies, positions, period):
    cycles = np.remainder(frequencies[:, None] * positions[None, :], period)
    return cycles * (2.0 * math.pi / period)


def interpolation(fine, coarse, bound, period):
    count = len(coarse)
    distance = fine[:, None] - coarse[None, :]
    total = np.ones_like(distance, dtype=np.float64)
    for frequency in range(1, bound):
        total += 2.0 * np.cos(np.remainder(frequency * distance, period) * (2.0 * math.pi / period))
    return total / count


def make_tables(strip_rows, margin, columns, freq_rows, freq_cols):
    window = strip_rows + 2 * margin
    row_freq = np.arange(freq_rows, dtype=np.float64) - freq_rows // 2
    col_freq = np.arange(freq_cols, dtype=np.float64) - freq_cols // 2
    rows_c, cols_c = 2 * freq_rows, 2 * freq_cols
    own = np.arange(margin, margin + strip_rows, dtype=np.float64)
    wide = np.arange(columns, dtype=np.float64)
    samples_r = np.arange(rows_c, dtype=np.float64) * (window / rows_c)
    samples_c = np.arange(cols_c, dtype=np.float64) * (columns / cols_c)
    factor = 1.0 / math.sqrt(window * columns)
    col_angle = angles(col_freq, wide[: columns // QUARTERS], columns)
    forward = np.concatenate([np.cos(col_angle).T, -np.sin(col_angle).T], axis=1) * factor
    row_angle = angles(row_freq, own, window)
    cos_r, sin_r = np.cos(row_angle), np.sin(row_angle)
    half = strip_rows // 2
    none = np.zeros((freq_rows, half))
    first = np.concatenate([cos_r[:, :half], none, sin_r[:, :half], none], axis=1)
    second = np.concatenate([none, cos_r[:, half:], none, sin_r[:, half:]], axis=1)
    project = np.concatenate([first, second], axis=0)
    back_rows = np.concatenate([cos_r, sin_r], axis=0).T
    coarse_r = angles(row_freq, samples_r, window)
    field_rows = np.concatenate([np.cos(coarse_r), np.sin(coarse_r)], axis=0).T
    coarse_c = angles(col_freq, samples_c, columns)
    cos_c, sin_c = np.cos(coarse_c), np.sin(coarse_c)
    field_cols = np.concatenate(
        [np.concatenate([cos_c, sin_c], axis=1), np.concatenate([-sin_c, cos_c], axis=1)], axis=0
    )
    widen_rows = interpolation(own, samples_r, freq_rows, window)
    widen_cols = interpolation(wide, samples_c, freq_cols, columns).T
    return {
        "forward": split_table(forward),
        "project": split_table(project),
        "back_rows": stack_left(back_rows),
        "field_rows": stack_left(field_rows),
        "field_rows_t": stack_left(field_rows.T),
        "field_cols": split_table(field_cols),
        "widen_rows": stack_left(widen_rows),
        "widen_rows_t": stack_left(widen_rows.T),
        "widen_cols": split_table(widen_cols),
    }


def split(value):
    high = value.astype(BF16)
    return high, (value - high.astype(F32)).astype(BF16)


def stack_right(value):
    high, low = split(value)
    return jnp.concatenate([high, low, high], axis=0)


def stack_turned(pair):
    high, low = (turn(piece, 1) for piece in split(pair))
    return jnp.concatenate([high, low, high], axis=0)


def dot(left, right):
    return jnp.dot(left, right, preferred_element_type=F32)


def dot_t(left, right):
    return lax.dot_general(left, right, (((1,), (1,)), ((), ())), preferred_element_type=F32)


def dot3(left, right):
    (lh, ll), (rh, rl) = left, right
    return dot(lh, rh) + dot(lh, rl) + dot(ll, rh)


def dot3_t(left, right):
    (lh, ll), (rh, rl) = left, right
    return dot_t(lh, rh) + dot_t(lh, rl) + dot_t(ll, rh)


def turn(pair, sign):
    half = pair.shape[1] // 2
    real, imag = pair[:, :half], pair[:, half:]
    if sign > 0:
        turned = jnp.concatenate([-imag, real], axis=1)
    else:
        turned = jnp.concatenate([imag, -real], axis=1)
    return jnp.concatenate([pair, turned], axis=0)


def alternate(shape):
    row = lax.broadcasted_iota(jnp.int32, shape, 0)
    return jnp.where(row % 2 == 0, 1.0, -1.0).astype(F32)


def is_first():
    return lax.axis_index("tiles") == 0


def is_last():
    return lax.axis_index("tiles") == lax.axis_size("tiles") - 1


def quarters(ref):
    width = ref.shape[1] // QUARTERS
    return [pl.ds(i * width, width) for i in range(QUARTERS)]


def quarter_turn(pair, count):
    half = pair.shape[1] // 2
    real, imag = pair[:, :half], pair[:, half:]
    lane = lax.broadcasted_iota(jnp.int32, (1, half), 1) - half // 2
    phase = (lane * count) & 3
    cosine = (phase == 0).astype(F32) - (phase == 2).astype(F32)
    sine = (phase == 1).astype(F32) - (phase == 3).astype(F32)
    return jnp.concatenate(
        [real * cosine - imag * sine, real * sine + imag * cosine], axis=1
    )


def project(
    mask_hbm, fwd_h_hbm, fwd_l_hbm, proj_h_hbm, proj_l_hbm, weights_hbm, slope_out, share_out, scratch
):
    mask, fwd_h, fwd_l, proj_h, proj_l, weights, sems = scratch
    columns = quarters(mask)
    masks = [
        pltpu.make_async_copy(mask_hbm.at[:, cols], mask.at[:, cols], sems.at[0, i])
        for i, cols in enumerate(columns)
    ]
    tables = [
        pltpu.make_async_copy(fwd_h_hbm, fwd_h, sems.at[1, 0]),
        pltpu.make_async_copy(fwd_l_hbm, fwd_l, sems.at[1, 1]),
    ]
    last = [
        pltpu.make_async_copy(weights_hbm, weights, sems.at[2, 2]),
        pltpu.make_async_copy(proj_h_hbm, proj_h, sems.at[2, 0]),
        pltpu.make_async_copy(proj_l_hbm, proj_l, sems.at[2, 1]),
    ]
    for copy in [masks[0], *tables, *masks[1:], *last]:
        copy.start()
    spectra = None
    for i, cols in enumerate(columns):
        masks[i].wait()
        transmit = jnp.tanh(mask[:, cols])
        slope_out[:, cols] = 1.0 - transmit * transmit
        pieces = split(transmit)
        if i == 0:
            for copy in tables:
                copy.wait()
        term = quarter_turn(dot3(pieces, (fwd_h[...], fwd_l[...])), -i)
        spectra = term if spectra is None else spectra + term
    for copy in last:
        copy.wait()
    kernels, width = share_out.shape
    whole = weights[0]
    for k in range(1, kernels):
        whole = whole + weights[k]
    rows = [jnp.full((1, width), weights[k], F32) for k in range(kernels)]
    share_out[...] = jnp.concatenate(rows, axis=0) / jnp.full((kernels, width), whole, F32)
    parts = dot3((proj_h[...], proj_l[...]), split(turn(spectra, -1)))
    half = parts.shape[0] // 2
    return parts[:half], parts[half:]


def project_first(*refs):
    args, (down, up, own, share, slope), scratch = refs[:6], refs[6:11], refs[11:]

    @pl.when(jnp.logical_not(is_last()))
    def _():
        low, high = project(*args, slope, share, scratch)
        down[...], up[...], own[...] = low, high, low + high


def project_second(*refs):
    args, taken, refs = refs[:6], refs[6:9], refs[10:]
    (near, up, own, share, slope), scratch = refs[:5], refs[5:]

    @pl.when(is_last())
    def _():
        low, high = project(*args, slope, share, scratch)
        near[...], up[...], own[...] = low, high, low + high

    @pl.when(jnp.logical_not(is_last()))
    def _():
        up[...], own[...], share[...] = (ref[...] for ref in taken)


def image(
    own, before, after, after_near, spectra, shares, target, rows_f, rows_t, cols_h, cols_l,
    wide_r, wide_rt, wide_h, wide_l, resist_hbm, grad_out, fields, resist_out, sem
):
    kernels, freq_rows, freq_cols = spectra.shape[1:]
    rows_c, cols_c = rows_f.shape[0], 2 * freq_cols
    group = math.gcd(kernels, GROUP)
    sign = alternate(own.shape)
    is_near = lax.axis_index("tiles") == lax.axis_size("tiles") - 2
    sides = before[...] + jnp.where(is_near, after_near[...], after[...])
    window = own[...] + sign * sides
    win_re, win_im = window[:, :freq_cols], window[:, freq_cols:]

    def forward(step, total):
        start = step * group
        inners = []
        for j in range(group):
            kern_re, kern_im = spectra[0, start + j], spectra[1, start + j]
            prod = jnp.concatenate(
                [kern_re * win_re - kern_im * win_im, kern_re * win_im + kern_im * win_re], axis=1
            )
            inners.append(dot(rows_f[...], stack_turned(prod)))
        inner = jnp.concatenate(inners, axis=0)
        field = dot3(split(inner), (cols_h[...], cols_l[...]))
        fields[pl.ds(pl.multiple_of(start * rows_c, rows_c), group * rows_c), :] = field
        power = field[:, :cols_c] ** 2 + field[:, cols_c:] ** 2
        for j in range(group):
            share = shares[pl.ds(start + j, 1), :]
            total = total + share * power[j * rows_c : (j + 1) * rows_c]
        return total

    total = lax.fori_loop(0, kernels // group, forward, jnp.zeros((rows_c, cols_c), F32))
    tall = dot(wide_r[...], stack_right(total))
    intensity = dot3(split(tall), (wide_h[...], wide_l[...]))
    resist = jax.nn.sigmoid(STEEPNESS * (intensity - THRESHOLD))
    resist_out[...] = resist
    sent = pltpu.make_async_copy(resist_out, resist_hbm, sem)
    sent.start()
    slopes = (4.0 * STEEPNESS) * (resist - target[...].astype(F32)) * resist * (1.0 - resist)
    narrow = dot3_t(split(slopes), (wide_h[...], wide_l[...]))
    weight = dot(wide_rt[...], stack_right(narrow))
    weight = jnp.concatenate([weight, weight], axis=1)

    def backward(step, sums):
        grad_re, grad_im = sums
        start = step * group
        scaled = jnp.concatenate(
            [
                weight * fields[pl.ds(pl.multiple_of((start + j) * rows_c, rows_c), rows_c), :]
                for j in range(group)
            ],
            axis=0,
        )
        inner = dot3_t(split(scaled), (cols_h[...], cols_l[...]))
        for j in range(group):
            spec = dot(rows_t[...], stack_right(inner[j * rows_c : (j + 1) * rows_c]))
            spec = shares[pl.ds(start + j, 1), :] * spec
            real = spec[:freq_rows, :freq_cols] + spec[freq_rows:, freq_cols:]
            imag = spec[:freq_rows, freq_cols:] - spec[freq_rows:, :freq_cols]
            kern_re, kern_im = spectra[0, start + j], spectra[1, start + j]
            grad_re = grad_re + real * kern_re + imag * kern_im
            grad_im = grad_im + imag * kern_re - real * kern_im
        return grad_re, grad_im

    none = jnp.zeros((freq_rows, freq_cols), F32)
    grad_re, grad_im = lax.fori_loop(0, kernels // group, backward, (none, none))
    grad_out[...] = jnp.concatenate([grad_re, grad_im], axis=1)
    sent.wait()


def image_first(*refs):
    @pl.when(jnp.logical_not(is_first()))
    def _():
        image(*refs)


def image_second(*refs):
    args, (_, grad_in), refs = refs[:15], refs[15:17], refs[17:]

    @pl.when(is_first())
    def _():
        image(*args, *refs)

    @pl.when(jnp.logical_not(is_first()))
    def _():
        refs[1][...] = grad_in[...]


def gradient_kernel(
    own, before, before_near, after, slope, rows_b, fwd_h, fwd_l, out_hbm, out, sems
):
    half = out.shape[0] // 2
    sign = alternate(own.shape)
    is_near = lax.axis_index("tiles") == 1
    low = stack_turned(own[...] + sign * jnp.where(is_near, before_near[...], before[...]))
    high = stack_turned(own[...] + sign * after[...])
    merged = jnp.concatenate([dot(rows_b[:half], low), dot(rows_b[half:], high)], axis=0)
    sent = []
    for i, cols in enumerate(quarters(out)):
        pieces = split(quarter_turn(merged, i))
        out[:, cols] = slope[:, cols] * dot3_t(pieces, (fwd_h[...], fwd_l[...]))
        sent.append(pltpu.make_async_copy(out.at[:, cols], out_hbm.at[:, cols], sems.at[i]))
        sent[-1].start()
    for copy in sent:
        copy.wait()


VMEM = pl.BlockSpec(memory_space=pltpu.VMEM)
HBM = pl.BlockSpec(memory_space=pltpu.HBM)


def call(kernel, outs, args, flops, scratch, out_specs, in_specs=None, aliases=None):
    shapes = [jax.ShapeDtypeStruct(shape, F32) for shape in outs]
    moved = sum(math.prod(a.shape) * a.dtype.itemsize for a in args)
    moved += sum(4 * math.prod(shape) for shape in outs)
    return pl.pallas_call(
        kernel,
        out_shape=shapes,
        in_specs=in_specs or [VMEM] * len(args),
        out_specs=out_specs,
        scratch_shapes=scratch,
        input_output_aliases=aliases or {},
        compiler_params=pltpu.CompilerParams(vmem_limit_bytes=LIMIT),
        cost_estimate=pl.CostEstimate(flops=flops, bytes_accessed=moved, transcendentals=0),
    )(*args)


def permute(value, pairs):
    return lax.ppermute(value, "tiles", pairs)


def shards(mask_params, target, kernel_spectra, kernel_weights):
    strip_rows, columns = mask_params.shape
    kernels, freq_rows, freq_cols = kernel_spectra.shape[1:]
    tables = jax.tree.map(
        jnp.asarray, make_tables(strip_rows, MARGIN, columns, freq_rows, freq_cols)
    )
    count = lax.axis_size("tiles")
    assert 2 * MARGIN == strip_rows and count % 2 == 0 and count > 2
    near_pairs = [(i, i ^ 1) for i in range(count)]
    up_pairs = [(i, (i + 1) % count) for i in range(count)]
    down_pairs = [(j, i) for i, j in up_pairs]
    pair, full, wide = (freq_rows, 2 * freq_cols), (strip_rows, columns), (kernels, 2 * freq_cols)
    area = strip_rows * columns

    args = [mask_params, *tables["forward"], *tables["project"]]
    held = [pltpu.VMEM(a.shape, a.dtype) for a in args]
    held += [pltpu.SMEM((kernels,), F32), pltpu.SemaphoreType.DMA((3, QUARTERS))]
    args.append(kernel_weights)
    args = [pltpu.with_memory_space_constraint(a, pltpu.HBM) for a in args]
    work = 60 * area * 2 * freq_cols
    send_down, send_up, own, share, slope = call(
        project_first, [pair, pair, pair, wide, full], args, work, held,
        in_specs=[HBM] * 6, out_specs=[VMEM] * 5,
    )
    after = permute(send_down, down_pairs)
    send_near, send_up, own, share, slope = call(
        project_second, [pair, pair, pair, wide, full], [*args, send_up, own, share, slope],
        work, held, in_specs=[HBM] * 6 + [VMEM] * 4, out_specs=[VMEM] * 5, aliases={9: 4},
    )
    before = permute(send_up, up_pairs)
    after_near = permute(send_near, near_pairs)

    rows_c, cols_c = 2 * freq_rows, 2 * freq_cols
    held = [
        pltpu.VMEM((kernels * rows_c, 2 * cols_c), F32),
        pltpu.VMEM(full, F32),
        pltpu.SemaphoreType.DMA,
    ]
    rest = [
        kernel_spectra, share, target,
        tables["field_rows"], tables["field_rows_t"], *tables["field_cols"],
        tables["widen_rows"], tables["widen_rows_t"], *tables["widen_cols"],
    ]
    specs = [VMEM] * 15
    work = 24 * kernels * rows_c * cols_c * cols_c
    resist, grad = call(
        image_first, [full, pair], [own, before, after, after_near, *rest], work, held,
        in_specs=specs, out_specs=[HBM, VMEM],
    )
    grad_before = permute(grad, up_pairs)
    resist, grad = call(
        image_second, [full, pair], [own, before, after, after_near, *rest, resist, grad], work, held,
        in_specs=specs + [HBM, VMEM], out_specs=[HBM, VMEM], aliases={15: 0},
    )
    grad_after = permute(grad, down_pairs)
    grad_before_near = permute(grad, near_pairs)
    (gradient,) = call(
        gradient_kernel,
        [full],
        [grad, grad_before, grad_before_near, grad_after, slope, tables["back_rows"], *tables["forward"]],
        6 * area * 2 * freq_cols,
        [pltpu.VMEM(full, F32), pltpu.SemaphoreType.DMA((QUARTERS,))],
        out_specs=[HBM],
    )
    return (resist, gradient)


def solution(mesh):
    in_specs = (P(("parts", "tiles"), None), P(("parts", "tiles"), None), P(), P())
    out_specs = (P(("parts", "tiles"), None), P(("parts", "tiles"), None))
    return jax.shard_map(shards, mesh=mesh, in_specs=in_specs, out_specs=out_specs, check_vma=False)
```

```python
import math

import jax
import jax.numpy as jnp
import numpy as np
from jax import lax
from jax.experimental import pallas as pl
from jax.experimental.pallas import tpu as pltpu
from jax.sharding import PartitionSpec as P


MARGIN = 64

STEEPNESS = 8.0
THRESHOLD = 0.35

BF16 = jnp.bfloat16
F32 = jnp.float32
QUARTERS = 4
GROUP = 8
LIMIT = 32 << 20


def split_table(table):
    table = np.asarray(table, np.float32)
    high = table.astype(BF16)
    low = (table - high.astype(np.float32)).astype(BF16)
    return high, low


def stack_left(table):
    high, low = split_table(table)
    return np.concatenate([high, high, low], axis=1)


def angles(frequencies, positions, period):
    cycles = np.remainder(frequencies[:, None] * positions[None, :], period)
    return cycles * (2.0 * math.pi / period)


def interpolation(fine, coarse, bound, period):
    count = len(coarse)
    distance = fine[:, None] - coarse[None, :]
    total = np.ones_like(distance, dtype=np.float64)
    for frequency in range(1, bound):
        total += 2.0 * np.cos(np.remainder(frequency * distance, period) * (2.0 * math.pi / period))
    return total / count


def make_tables(strip_rows, margin, columns, freq_rows, freq_cols):
    window = strip_rows + 2 * margin
    row_freq = np.arange(freq_rows, dtype=np.float64) - freq_rows // 2
    col_freq = np.arange(freq_cols, dtype=np.float64) - freq_cols // 2
    rows_c, cols_c = 2 * freq_rows, 2 * freq_cols
    own = np.arange(margin, margin + strip_rows, dtype=np.float64)
    wide = np.arange(columns, dtype=np.float64)
    samples_r = np.arange(rows_c, dtype=np.float64) * (window / rows_c)
    samples_c = np.arange(cols_c, dtype=np.float64) * (columns / cols_c)
    factor = 1.0 / math.sqrt(window * columns)
    col_angle = angles(col_freq, wide[: columns // QUARTERS], columns)
    forward = np.concatenate([np.cos(col_angle).T, -np.sin(col_angle).T], axis=1) * factor
    row_angle = angles(row_freq, own, window)
    cos_r, sin_r = np.cos(row_angle), np.sin(row_angle)
    half = strip_rows // 2
    none = np.zeros((freq_rows, half))
    first = np.concatenate([cos_r[:, :half], none, sin_r[:, :half], none], axis=1)
    second = np.concatenate([none, cos_r[:, half:], none, sin_r[:, half:]], axis=1)
    project = np.concatenate([first, second], axis=0)
    back_rows = np.concatenate([cos_r, sin_r], axis=0).T
    coarse_r = angles(row_freq, samples_r, window)
    field_rows = np.concatenate([np.cos(coarse_r), np.sin(coarse_r)], axis=0).T
    coarse_c = angles(col_freq, samples_c, columns)
    cos_c, sin_c = np.cos(coarse_c), np.sin(coarse_c)
    field_cols = np.concatenate(
        [np.concatenate([cos_c, sin_c], axis=1), np.concatenate([-sin_c, cos_c], axis=1)], axis=0
    )
    widen_rows = interpolation(own, samples_r, freq_rows, window)
    widen_cols = interpolation(wide, samples_c, freq_cols, columns).T
    return {
        "forward": split_table(forward),
        "project": split_table(project),
        "back_rows": stack_left(back_rows),
        "field_rows": stack_left(field_rows),
        "field_rows_t": stack_left(field_rows.T),
        "field_cols": split_table(field_cols),
        "widen_rows": stack_left(widen_rows),
        "widen_rows_t": stack_left(widen_rows.T),
        "widen_cols": split_table(widen_cols),
    }


def split(value):
    high = value.astype(BF16)
    return high, (value - high.astype(F32)).astype(BF16)


def stack_right(value):
    high, low = split(value)
    return jnp.concatenate([high, low, high], axis=0)


def stack_turned(pair):
    high, low = (turn(piece, 1) for piece in split(pair))
    return jnp.concatenate([high, low, high], axis=0)


def dot(left, right):
    return jnp.dot(left, right, preferred_element_type=F32)


def dot_t(left, right):
    return lax.dot_general(left, right, (((1,), (1,)), ((), ())), preferred_element_type=F32)


def dot3(left, right):
    (lh, ll), (rh, rl) = left, right
    return dot(lh, rh) + dot(lh, rl) + dot(ll, rh)


def dot3_t(left, right):
    (lh, ll), (rh, rl) = left, right
    return dot_t(lh, rh) + dot_t(lh, rl) + dot_t(ll, rh)


def turn(pair, sign):
    half = pair.shape[1] // 2
    real, imag = pair[:, :half], pair[:, half:]
    if sign > 0:
        turned = jnp.concatenate([-imag, real], axis=1)
    else:
        turned = jnp.concatenate([imag, -real], axis=1)
    return jnp.concatenate([pair, turned], axis=0)


def alternate(shape):
    row = lax.broadcasted_iota(jnp.int32, shape, 0)
    return jnp.where(row % 2 == 0, 1.0, -1.0).astype(F32)


def is_first():
    return lax.axis_index("tiles") == 0


def is_last():
    return lax.axis_index("tiles") == lax.axis_size("tiles") - 1


def is_odd():
    return lax.axis_index("tiles") % 2 == 1


def quarters(ref):
    width = ref.shape[1] // QUARTERS
    return [pl.ds(i * width, width) for i in range(QUARTERS)]


def quarter_turn(pair, count):
    half = pair.shape[1] // 2
    real, imag = pair[:, :half], pair[:, half:]
    lane = lax.broadcasted_iota(jnp.int32, (1, half), 1) - half // 2
    phase = (lane * count) & 3
    cosine = (phase == 0).astype(F32) - (phase == 2).astype(F32)
    sine = (phase == 1).astype(F32) - (phase == 3).astype(F32)
    return jnp.concatenate(
        [real * cosine - imag * sine, real * sine + imag * cosine], axis=1
    )


def project(
    mask_hbm, fwd_h_hbm, fwd_l_hbm, proj_h_hbm, proj_l_hbm, weights_hbm, slope_out, share_out, scratch
):
    mask, fwd_h, fwd_l, proj_h, proj_l, weights, sems = scratch
    columns = quarters(mask)
    masks = [
        pltpu.make_async_copy(mask_hbm.at[:, cols], mask.at[:, cols], sems.at[0, i])
        for i, cols in enumerate(columns)
    ]
    tables = [
        pltpu.make_async_copy(fwd_h_hbm, fwd_h, sems.at[1, 0]),
        pltpu.make_async_copy(fwd_l_hbm, fwd_l, sems.at[1, 1]),
    ]
    last = [
        pltpu.make_async_copy(weights_hbm, weights, sems.at[2, 2]),
        pltpu.make_async_copy(proj_h_hbm, proj_h, sems.at[2, 0]),
        pltpu.make_async_copy(proj_l_hbm, proj_l, sems.at[2, 1]),
    ]
    for copy in [masks[0], *tables, *masks[1:], *last]:
        copy.start()
    spectra = None
    for i, cols in enumerate(columns):
        masks[i].wait()
        transmit = jnp.tanh(mask[:, cols])
        slope_out[:, cols] = 1.0 - transmit * transmit
        pieces = split(transmit)
        if i == 0:
            for copy in tables:
                copy.wait()
        term = quarter_turn(dot3(pieces, (fwd_h[...], fwd_l[...])), -i)
        spectra = term if spectra is None else spectra + term
    for copy in last:
        copy.wait()
    kernels, width = share_out.shape
    whole = weights[0]
    for k in range(1, kernels):
        whole = whole + weights[k]
    rows = [jnp.full((1, width), weights[k], F32) for k in range(kernels)]
    share_out[...] = jnp.concatenate(rows, axis=0) / jnp.full((kernels, width), whole, F32)
    parts = dot3((proj_h[...], proj_l[...]), split(turn(spectra, -1)))
    half = parts.shape[0] // 2
    return parts[:half], parts[half:]


def project_first(*refs):
    args, (far, near, own, share, slope), scratch = refs[:6], refs[6:11], refs[11:]

    @pl.when(jnp.logical_not(is_last()))
    def _():
        low, high = project(*args, slope, share, scratch)
        odd = is_odd()
        far[...] = jnp.where(odd, high, low)
        near[...] = jnp.where(odd, low, high)
        own[...] = low + high


def project_second(*refs):
    args, taken, refs = refs[:6], refs[6:10], refs[11:]
    (far, near, own, share, slope), scratch = refs[:5], refs[5:]

    @pl.when(is_last())
    def _():
        low, high = project(*args, slope, share, scratch)
        far[...], near[...], own[...] = high, low, low + high

    @pl.when(jnp.logical_not(is_last()))
    def _():
        far[...], near[...], own[...], share[...] = (ref[...] for ref in taken)


def image(
    own, far, near, spectra, shares, target, rows_f, rows_t, cols_h, cols_l,
    wide_r, wide_rt, wide_h, wide_l, resist_hbm, grad_out, fields, resist_out, sem
):
    kernels, freq_rows, freq_cols = spectra.shape[1:]
    rows_c, cols_c = rows_f.shape[0], 2 * freq_cols
    group = math.gcd(kernels, GROUP)
    sign = alternate(own.shape)
    window = own[...] + sign * (far[...] + near[...])
    win_re, win_im = window[:, :freq_cols], window[:, freq_cols:]

    def forward(step, total):
        start = step * group
        inners = []
        for j in range(group):
            kern_re, kern_im = spectra[0, start + j], spectra[1, start + j]
            prod = jnp.concatenate(
                [kern_re * win_re - kern_im * win_im, kern_re * win_im + kern_im * win_re], axis=1
            )
            inners.append(dot(rows_f[...], stack_turned(prod)))
        inner = jnp.concatenate(inners, axis=0)
        field = dot3(split(inner), (cols_h[...], cols_l[...]))
        fields[pl.ds(pl.multiple_of(start * rows_c, rows_c), group * rows_c), :] = field
        power = field[:, :cols_c] ** 2 + field[:, cols_c:] ** 2
        for j in range(group):
            share = shares[pl.ds(start + j, 1), :]
            total = total + share * power[j * rows_c : (j + 1) * rows_c]
        return total

    total = lax.fori_loop(0, kernels // group, forward, jnp.zeros((rows_c, cols_c), F32))
    tall = dot(wide_r[...], stack_right(total))
    intensity = dot3(split(tall), (wide_h[...], wide_l[...]))
    resist = jax.nn.sigmoid(STEEPNESS * (intensity - THRESHOLD))
    resist_out[...] = resist
    sent = pltpu.make_async_copy(resist_out, resist_hbm, sem)
    sent.start()
    slopes = (4.0 * STEEPNESS) * (resist - target[...].astype(F32)) * resist * (1.0 - resist)
    narrow = dot3_t(split(slopes), (wide_h[...], wide_l[...]))
    weight = dot(wide_rt[...], stack_right(narrow))
    weight = jnp.concatenate([weight, weight], axis=1)

    def backward(step, sums):
        grad_re, grad_im = sums
        start = step * group
        scaled = jnp.concatenate(
            [
                weight * fields[pl.ds(pl.multiple_of((start + j) * rows_c, rows_c), rows_c), :]
                for j in range(group)
            ],
            axis=0,
        )
        inner = dot3_t(split(scaled), (cols_h[...], cols_l[...]))
        for j in range(group):
            spec = dot(rows_t[...], stack_right(inner[j * rows_c : (j + 1) * rows_c]))
            spec = shares[pl.ds(start + j, 1), :] * spec
            real = spec[:freq_rows, :freq_cols] + spec[freq_rows:, freq_cols:]
            imag = spec[:freq_rows, freq_cols:] - spec[freq_rows:, :freq_cols]
            kern_re, kern_im = spectra[0, start + j], spectra[1, start + j]
            grad_re = grad_re + real * kern_re + imag * kern_im
            grad_im = grad_im + imag * kern_re - real * kern_im
        return grad_re, grad_im

    none = jnp.zeros((freq_rows, freq_cols), F32)
    grad_re, grad_im = lax.fori_loop(0, kernels // group, backward, (none, none))
    grad_out[...] = jnp.concatenate([grad_re, grad_im], axis=1)
    sent.wait()


def image_first(*refs):
    @pl.when(jnp.logical_not(is_first()))
    def _():
        image(*refs)


def image_second(*refs):
    args, (_, grad_in), refs = refs[:14], refs[14:16], refs[16:]

    @pl.when(is_first())
    def _():
        image(*args, *refs)

    @pl.when(jnp.logical_not(is_first()))
    def _():
        refs[1][...] = grad_in[...]


def gradient_kernel(
    own, before_even, before_odd, after, slope, rows_b, fwd_h, fwd_l, out_hbm, out, sems
):
    half = out.shape[0] // 2
    sign = alternate(own.shape)
    before = jnp.where(is_odd(), before_odd[...], before_even[...])
    low = stack_turned(own[...] + sign * before)
    high = stack_turned(own[...] + sign * after[...])
    merged = jnp.concatenate([dot(rows_b[:half], low), dot(rows_b[half:], high)], axis=0)
    sent = []
    for i, cols in enumerate(quarters(out)):
        pieces = split(quarter_turn(merged, i))
        out[:, cols] = slope[:, cols] * dot3_t(pieces, (fwd_h[...], fwd_l[...]))
        sent.append(pltpu.make_async_copy(out.at[:, cols], out_hbm.at[:, cols], sems.at[i]))
        sent[-1].start()
    for copy in sent:
        copy.wait()


VMEM = pl.BlockSpec(memory_space=pltpu.VMEM)
HBM = pl.BlockSpec(memory_space=pltpu.HBM)


def call(kernel, outs, args, flops, scratch, out_specs, in_specs=None, aliases=None):
    shapes = [jax.ShapeDtypeStruct(shape, F32) for shape in outs]
    moved = sum(math.prod(a.shape) * a.dtype.itemsize for a in args)
    moved += sum(4 * math.prod(shape) for shape in outs)
    return pl.pallas_call(
        kernel,
        out_shape=shapes,
        in_specs=in_specs or [VMEM] * len(args),
        out_specs=out_specs,
        scratch_shapes=scratch,
        input_output_aliases=aliases or {},
        compiler_params=pltpu.CompilerParams(vmem_limit_bytes=LIMIT),
        cost_estimate=pl.CostEstimate(flops=flops, bytes_accessed=moved, transcendentals=0),
    )(*args)


def permute(value, pairs):
    return lax.ppermute(value, "tiles", pairs)


def shards(mask_params, target, kernel_spectra, kernel_weights):
    strip_rows, columns = mask_params.shape
    kernels, freq_rows, freq_cols = kernel_spectra.shape[1:]
    tables = jax.tree.map(
        jnp.asarray, make_tables(strip_rows, MARGIN, columns, freq_rows, freq_cols)
    )
    count = lax.axis_size("tiles")
    assert 2 * MARGIN == strip_rows and count % 2 == 0 and count >= 6
    near_pairs = [(i, i ^ 1) for i in range(count)]
    far_pairs = [(i, (i + 1 if i % 2 else i - 1) % count) for i in range(count)]
    last = count - 1
    ends = [(last, 0), (0, last - 1), (last - 1, last), (1, 2), (2, 3), (3, 1)]
    wrap1_pairs = ends + near_pairs[4 : last - 1]
    wrap2_pairs = [(last, 0), (0, 1), (1, 2), (2, last)] + far_pairs[3:last]
    down_pairs = [(i, (i - 1) % count) for i in range(count)]
    pair, full, wide = (freq_rows, 2 * freq_cols), (strip_rows, columns), (kernels, 2 * freq_cols)
    area = strip_rows * columns

    args = [mask_params, *tables["forward"], *tables["project"]]
    held = [pltpu.VMEM(a.shape, a.dtype) for a in args]
    held += [pltpu.SMEM((kernels,), F32), pltpu.SemaphoreType.DMA((3, QUARTERS))]
    args.append(kernel_weights)
    args = [pltpu.with_memory_space_constraint(a, pltpu.HBM) for a in args]
    work = 60 * area * 2 * freq_cols
    send_far, send_near, own, share, slope = call(
        project_first, [pair, pair, pair, wide, full], args, work, held,
        in_specs=[HBM] * 6, out_specs=[VMEM] * 5,
    )
    far = permute(send_far, far_pairs)
    send_far, send_near, own, share, slope = call(
        project_second, [pair, pair, pair, wide, full],
        [*args, send_far, send_near, own, share, slope],
        work, held, in_specs=[HBM] * 6 + [VMEM] * 5, out_specs=[VMEM] * 5, aliases={10: 4},
    )
    near = permute(send_near, near_pairs)
    far_first = permute(send_far, wrap1_pairs)

    rows_c, cols_c = 2 * freq_rows, 2 * freq_cols
    held = [
        pltpu.VMEM((kernels * rows_c, 2 * cols_c), F32),
        pltpu.VMEM(full, F32),
        pltpu.SemaphoreType.DMA,
    ]
    rest = [
        kernel_spectra, share, target,
        tables["field_rows"], tables["field_rows_t"], *tables["field_cols"],
        tables["widen_rows"], tables["widen_rows_t"], *tables["widen_cols"],
    ]
    specs = [VMEM] * 14
    work = 24 * kernels * rows_c * cols_c * cols_c
    resist, grad = call(
        image_first, [full, pair], [own, far, near, *rest], work, held,
        in_specs=specs, out_specs=[HBM, VMEM],
    )
    grad_before_even = permute(grad, wrap2_pairs)
    resist, grad = call(
        image_second, [full, pair], [own, far_first, near, *rest, resist, grad], work, held,
        in_specs=specs + [HBM, VMEM], out_specs=[HBM, VMEM], aliases={14: 0},
    )
    grad_after = permute(grad, down_pairs)
    grad_before_odd = permute(grad, near_pairs)
    (gradient,) = call(
        gradient_kernel,
        [full],
        [
            grad, grad_before_even, grad_before_odd, grad_after, slope,
            tables["back_rows"], *tables["forward"],
        ],
        6 * area * 2 * freq_cols,
        [pltpu.VMEM(full, F32), pltpu.SemaphoreType.DMA((QUARTERS,))],
        out_specs=[HBM],
    )
    return (resist, gradient)


def solution(mesh):
    in_specs = (P(("parts", "tiles"), None), P(("parts", "tiles"), None), P(), P())
    out_specs = (P(("parts", "tiles"), None), P(("parts", "tiles"), None))
    return jax.shard_map(shards, mesh=mesh, in_specs=in_specs, out_specs=out_specs, check_vma=False)
```

```python
import math

import jax
import jax.numpy as jnp
import numpy as np
from jax import lax
from jax.experimental import pallas as pl
from jax.experimental.pallas import tpu as pltpu
from jax.sharding import PartitionSpec as P


MARGIN = 64

STEEPNESS = 8.0
THRESHOLD = 0.35

BF16 = jnp.bfloat16
F32 = jnp.float32
QUARTERS = 4
GROUP = 8
LIMIT = 32 << 20


def split_table(table):
    table = np.asarray(table, np.float32)
    high = table.astype(BF16)
    low = (table - high.astype(np.float32)).astype(BF16)
    return high, low


def stack_left(table):
    high, low = split_table(table)
    return np.concatenate([high, high, low], axis=1)


def stack_both(table):
    high, low = split_table(table)
    return np.concatenate(
        [np.concatenate([high, high], axis=1), np.concatenate([low, 0 * low], axis=1)], axis=0
    )


def angles(frequencies, positions, period):
    cycles = np.remainder(frequencies[:, None] * positions[None, :], period)
    return cycles * (2.0 * math.pi / period)


def interpolation(fine, coarse, bound, period):
    count = len(coarse)
    distance = fine[:, None] - coarse[None, :]
    total = np.ones_like(distance, dtype=np.float64)
    for frequency in range(1, bound):
        total += 2.0 * np.cos(np.remainder(frequency * distance, period) * (2.0 * math.pi / period))
    return total / count


def make_tables(strip_rows, margin, columns, freq_rows, freq_cols):
    window = strip_rows + 2 * margin
    row_freq = np.arange(freq_rows, dtype=np.float64) - freq_rows // 2
    col_freq = np.arange(freq_cols, dtype=np.float64) - freq_cols // 2
    rows_c, cols_c = 2 * freq_rows, 2 * freq_cols
    own = np.arange(margin, margin + strip_rows, dtype=np.float64)
    wide = np.arange(columns, dtype=np.float64)
    samples_r = np.arange(rows_c, dtype=np.float64) * (window / rows_c)
    samples_c = np.arange(cols_c, dtype=np.float64) * (columns / cols_c)
    factor = 1.0 / math.sqrt(window * columns)
    col_angle = angles(col_freq, wide[: columns // QUARTERS], columns)
    forward = np.concatenate([np.cos(col_angle).T, -np.sin(col_angle).T], axis=1) * factor
    row_angle = angles(row_freq, own, window)
    cos_r, sin_r = np.cos(row_angle), np.sin(row_angle)
    half = strip_rows // 2
    none = np.zeros((freq_rows, half))
    first = np.concatenate([cos_r[:, :half], none, sin_r[:, :half], none], axis=1)
    second = np.concatenate([none, cos_r[:, half:], none, sin_r[:, half:]], axis=1)
    project = np.concatenate([first, second], axis=0)
    back_rows = np.concatenate([cos_r, sin_r], axis=0).T
    coarse_r = angles(row_freq, samples_r, window)
    cos_f, sin_f = np.cos(coarse_r).T, np.sin(coarse_r).T
    field_rows = np.concatenate(
        [np.concatenate([cos_f, -sin_f], axis=1), np.concatenate([sin_f, cos_f], axis=1)], axis=0
    )
    coarse_c = angles(col_freq, samples_c, columns)
    cos_c, sin_c = np.cos(coarse_c), np.sin(coarse_c)
    field_cols = np.concatenate(
        [np.concatenate([cos_c, sin_c], axis=1), np.concatenate([-sin_c, cos_c], axis=1)], axis=0
    )
    widen_rows = interpolation(own, samples_r, freq_rows, window)
    widen_cols = interpolation(wide, samples_c, freq_cols, columns).T
    return {
        "forward": split_table(forward),
        "project": split_table(project),
        "back_rows": stack_left(back_rows),
        "field_rows": stack_left(field_rows),
        "field_rows_t": stack_both(field_rows.T),
        "field_cols": split_table(field_cols),
        "widen_rows": stack_left(widen_rows),
        "widen_rows_t": stack_left(widen_rows.T),
        "widen_cols": split_table(widen_cols),
    }


def split(value):
    high = value.astype(BF16)
    return high, (value - high.astype(F32)).astype(BF16)


def stack_right(value):
    high, low = split(value)
    return jnp.concatenate([high, low, high], axis=0)


def stack_turned(pair):
    high, low = (turn(piece, 1) for piece in split(pair))
    return jnp.concatenate([high, low, high], axis=0)


def dot(left, right):
    return jnp.dot(left, right, preferred_element_type=F32)


def dot_t(left, right):
    return lax.dot_general(left, right, (((1,), (1,)), ((), ())), preferred_element_type=F32)


def dot3(left, right):
    (lh, ll), (rh, rl) = left, right
    return dot(lh, rh) + dot(lh, rl) + dot(ll, rh)


def dot3_t(left, right):
    (lh, ll), (rh, rl) = left, right
    return dot_t(lh, rh) + dot_t(lh, rl) + dot_t(ll, rh)


def turn(pair, sign):
    half = pair.shape[1] // 2
    real, imag = pair[:, :half], pair[:, half:]
    if sign > 0:
        turned = jnp.concatenate([-imag, real], axis=1)
    else:
        turned = jnp.concatenate([imag, -real], axis=1)
    return jnp.concatenate([pair, turned], axis=0)


def alternate(shape):
    row = lax.broadcasted_iota(jnp.int32, shape, 0)
    return jnp.where(row % 2 == 0, 1.0, -1.0).astype(F32)


def is_first():
    return lax.axis_index("tiles") == 0


def is_last():
    return lax.axis_index("tiles") == lax.axis_size("tiles") - 1


def is_odd():
    return lax.axis_index("tiles") % 2 == 1


def quarters(ref):
    width = ref.shape[1] // QUARTERS
    return [pl.ds(i * width, width) for i in range(QUARTERS)]


def quarter_turn(pair, count):
    half = pair.shape[1] // 2
    real, imag = pair[:, :half], pair[:, half:]
    lane = lax.broadcasted_iota(jnp.int32, (1, half), 1) - half // 2
    phase = (lane * count) & 3
    cosine = (phase == 0).astype(F32) - (phase == 2).astype(F32)
    sine = (phase == 1).astype(F32) - (phase == 3).astype(F32)
    return jnp.concatenate(
        [real * cosine - imag * sine, real * sine + imag * cosine], axis=1
    )


def project(
    mask_hbm, fwd_h_hbm, fwd_l_hbm, proj_h_hbm, proj_l_hbm, weights_hbm, slope_out, share_out, scratch
):
    mask, fwd_h, fwd_l, proj_h, proj_l, weights, sems = scratch
    columns = quarters(mask)
    masks = [
        pltpu.make_async_copy(mask_hbm.at[:, cols], mask.at[:, cols], sems.at[0, i])
        for i, cols in enumerate(columns)
    ]
    tables = [
        pltpu.make_async_copy(fwd_h_hbm, fwd_h, sems.at[1, 0]),
        pltpu.make_async_copy(fwd_l_hbm, fwd_l, sems.at[1, 1]),
    ]
    last = [
        pltpu.make_async_copy(weights_hbm, weights, sems.at[2, 2]),
        pltpu.make_async_copy(proj_h_hbm, proj_h, sems.at[2, 0]),
        pltpu.make_async_copy(proj_l_hbm, proj_l, sems.at[2, 1]),
    ]
    for copy in [masks[0], *tables, *masks[1:], *last]:
        copy.start()
    spectra = None
    for i, cols in enumerate(columns):
        masks[i].wait()
        transmit = jnp.tanh(mask[:, cols])
        slope_out[:, cols] = 1.0 - transmit * transmit
        pieces = split(transmit)
        if i == 0:
            for copy in tables:
                copy.wait()
        term = quarter_turn(dot3(pieces, (fwd_h[...], fwd_l[...])), -i)
        spectra = term if spectra is None else spectra + term
    for copy in last:
        copy.wait()
    kernels, width = share_out.shape
    whole = weights[0]
    for k in range(1, kernels):
        whole = whole + weights[k]
    rows = [jnp.full((1, width), weights[k], F32) for k in range(kernels)]
    share_out[...] = jnp.concatenate(rows, axis=0) / jnp.full((kernels, width), whole, F32)
    parts = dot3((proj_h[...], proj_l[...]), split(turn(spectra, -1)))
    half = parts.shape[0] // 2
    return parts[:half], parts[half:]


def project_first(*refs):
    args, (far, near, own, share, slope), scratch = refs[:6], refs[6:11], refs[11:]

    @pl.when(jnp.logical_not(is_last()))
    def _():
        low, high = project(*args, slope, share, scratch)
        odd = is_odd()
        far[...] = jnp.where(odd, high, low)
        near[...] = jnp.where(odd, low, high)
        own[...] = low + high


def project_second(*refs):
    args, taken, refs = refs[:6], refs[6:10], refs[11:]
    (far, near, own, share, slope), scratch = refs[:5], refs[5:]

    @pl.when(is_last())
    def _():
        low, high = project(*args, slope, share, scratch)
        far[...], near[...], own[...] = high, low, low + high

    @pl.when(jnp.logical_not(is_last()))
    def _():
        far[...], near[...], own[...], share[...] = (ref[...] for ref in taken)


def image(
    own, far, near, spectra, shares, target, rows_f, rows_t, cols_h, cols_l,
    wide_r, wide_rt, wide_h, wide_l, resist_hbm, grad_out, fields, resist_out, sem
):
    kernels, freq_rows, freq_cols = spectra.shape[1:]
    rows_c, cols_c = rows_f.shape[0] // 2, 2 * freq_cols
    group = math.gcd(kernels, GROUP)
    sign = alternate(own.shape)
    window = own[...] + sign * (far[...] + near[...])
    win_re, win_im = window[:, :freq_cols], window[:, freq_cols:]

    def forward(step, total):
        start = step * group
        prods = []
        for j in range(group):
            kern_re, kern_im = spectra[0, start + j], spectra[1, start + j]
            prods.append(jnp.concatenate(
                [kern_re * win_re - kern_im * win_im, kern_re * win_im + kern_im * win_re], axis=1
            ))
        inner = dot3(split(jnp.concatenate(prods, axis=0)), (cols_h[...], cols_l[...]))
        for j in range(group):
            part = inner[j * freq_rows : (j + 1) * freq_rows]
            part = jnp.concatenate([part[:, :cols_c], part[:, cols_c:]], axis=0)
            field = dot(rows_f[...], stack_right(part))
            fields[start + j] = field
            power = field[:rows_c] ** 2 + field[rows_c:] ** 2
            total = total + shares[pl.ds(start + j, 1), :] * power
        return total

    total = lax.fori_loop(0, kernels // group, forward, jnp.zeros((rows_c, cols_c), F32))
    tall = dot(wide_r[...], stack_right(total))
    intensity = dot3(split(tall), (wide_h[...], wide_l[...]))
    resist = jax.nn.sigmoid(STEEPNESS * (intensity - THRESHOLD))
    resist_out[...] = resist
    sent = pltpu.make_async_copy(resist_out, resist_hbm, sem)
    sent.start()
    slopes = (4.0 * STEEPNESS) * (resist - target[...].astype(F32)) * resist * (1.0 - resist)
    narrow = dot3_t(split(slopes), (wide_h[...], wide_l[...]))
    weight = dot(wide_rt[...], stack_right(narrow))
    weight = jnp.concatenate([weight, weight], axis=0)

    def backward(step, sums):
        grad_re, grad_im = sums
        start = step * group
        inners = []
        for j in range(group):
            pieces = jnp.concatenate(split(weight * fields[start + j]), axis=0)
            part = dot(rows_t[...], pieces)
            part = part[: 2 * freq_rows] + part[2 * freq_rows :]
            inners.append(jnp.concatenate([part[:freq_rows], part[freq_rows:]], axis=1))
        spec = dot3_t(split(jnp.concatenate(inners, axis=0)), (cols_h[...], cols_l[...]))
        for j in range(group):
            part = shares[pl.ds(start + j, 1), :] * spec[j * freq_rows : (j + 1) * freq_rows]
            real, imag = part[:, :freq_cols], part[:, freq_cols:]
            kern_re, kern_im = spectra[0, start + j], spectra[1, start + j]
            grad_re = grad_re + real * kern_re + imag * kern_im
            grad_im = grad_im + imag * kern_re - real * kern_im
        return grad_re, grad_im

    none = jnp.zeros((freq_rows, freq_cols), F32)
    grad_re, grad_im = lax.fori_loop(0, kernels // group, backward, (none, none))
    grad_out[...] = jnp.concatenate([grad_re, grad_im], axis=1)
    sent.wait()


def image_first(*refs):
    @pl.when(jnp.logical_not(is_first()))
    def _():
        image(*refs)


def image_second(*refs):
    args, (_, grad_in), refs = refs[:14], refs[14:16], refs[16:]

    @pl.when(is_first())
    def _():
        image(*args, *refs)

    @pl.when(jnp.logical_not(is_first()))
    def _():
        refs[1][...] = grad_in[...]


def gradient_kernel(
    own, before_even, before_odd, after, slope, rows_b, fwd_h, fwd_l, out_hbm, out, sems
):
    half = out.shape[0] // 2
    sign = alternate(own.shape)
    before = jnp.where(is_odd(), before_odd[...], before_even[...])
    low = stack_turned(own[...] + sign * before)
    high = stack_turned(own[...] + sign * after[...])
    merged = jnp.concatenate([dot(rows_b[:half], low), dot(rows_b[half:], high)], axis=0)
    sent = []
    for i, cols in enumerate(quarters(out)):
        pieces = split(quarter_turn(merged, i))
        out[:, cols] = slope[:, cols] * dot3_t(pieces, (fwd_h[...], fwd_l[...]))
        sent.append(pltpu.make_async_copy(out.at[:, cols], out_hbm.at[:, cols], sems.at[i]))
        sent[-1].start()
    for copy in sent:
        copy.wait()


VMEM = pl.BlockSpec(memory_space=pltpu.VMEM)
HBM = pl.BlockSpec(memory_space=pltpu.HBM)


def call(kernel, outs, args, flops, scratch, out_specs, in_specs=None, aliases=None):
    shapes = [jax.ShapeDtypeStruct(shape, F32) for shape in outs]
    moved = sum(math.prod(a.shape) * a.dtype.itemsize for a in args)
    moved += sum(4 * math.prod(shape) for shape in outs)
    return pl.pallas_call(
        kernel,
        out_shape=shapes,
        in_specs=in_specs or [VMEM] * len(args),
        out_specs=out_specs,
        scratch_shapes=scratch,
        input_output_aliases=aliases or {},
        compiler_params=pltpu.CompilerParams(vmem_limit_bytes=LIMIT),
        cost_estimate=pl.CostEstimate(flops=flops, bytes_accessed=moved, transcendentals=0),
    )(*args)


def permute(value, pairs):
    return lax.ppermute(value, "tiles", pairs)


def shards(mask_params, target, kernel_spectra, kernel_weights):
    strip_rows, columns = mask_params.shape
    kernels, freq_rows, freq_cols = kernel_spectra.shape[1:]
    tables = jax.tree.map(
        jnp.asarray, make_tables(strip_rows, MARGIN, columns, freq_rows, freq_cols)
    )
    count = lax.axis_size("tiles")
    assert 2 * MARGIN == strip_rows and count % 2 == 0 and count >= 6
    near_pairs = [(i, i ^ 1) for i in range(count)]
    far_pairs = [(i, (i + 1 if i % 2 else i - 1) % count) for i in range(count)]
    last = count - 1
    ends = [(last, 0), (0, last - 1), (last - 1, last), (1, 2), (2, 3), (3, 1)]
    wrap1_pairs = ends + near_pairs[4 : last - 1]
    wrap2_pairs = [(last, 0), (0, 1), (1, 2), (2, last)] + far_pairs[3:last]
    down_pairs = [(i, (i - 1) % count) for i in range(count)]
    pair, full, wide = (freq_rows, 2 * freq_cols), (strip_rows, columns), (kernels, 2 * freq_cols)
    area = strip_rows * columns

    args = [mask_params, *tables["forward"], *tables["project"]]
    held = [pltpu.VMEM(a.shape, a.dtype) for a in args]
    held += [pltpu.SMEM((kernels,), F32), pltpu.SemaphoreType.DMA((3, QUARTERS))]
    args.append(kernel_weights)
    args = [pltpu.with_memory_space_constraint(a, pltpu.HBM) for a in args]
    work = 60 * area * 2 * freq_cols
    send_far, send_near, own, share, slope = call(
        project_first, [pair, pair, pair, wide, full], args, work, held,
        in_specs=[HBM] * 6, out_specs=[VMEM] * 5,
    )
    far = permute(send_far, far_pairs)
    send_far, send_near, own, share, slope = call(
        project_second, [pair, pair, pair, wide, full],
        [*args, send_far, send_near, own, share, slope],
        work, held, in_specs=[HBM] * 6 + [VMEM] * 5, out_specs=[VMEM] * 5, aliases={10: 4},
    )
    near = permute(send_near, near_pairs)
    far_first = permute(send_far, wrap1_pairs)

    rows_c, cols_c = 2 * freq_rows, 2 * freq_cols
    held = [
        pltpu.VMEM((kernels, 2 * rows_c, cols_c), F32),
        pltpu.VMEM(full, F32),
        pltpu.SemaphoreType.DMA,
    ]
    rest = [
        kernel_spectra, share, target,
        tables["field_rows"], tables["field_rows_t"], *tables["field_cols"],
        tables["widen_rows"], tables["widen_rows_t"], *tables["widen_cols"],
    ]
    specs = [VMEM] * 14
    work = 24 * kernels * rows_c * cols_c * cols_c
    resist, grad = call(
        image_first, [full, pair], [own, far, near, *rest], work, held,
        in_specs=specs, out_specs=[HBM, VMEM],
    )
    grad_before_even = permute(grad, wrap2_pairs)
    resist, grad = call(
        image_second, [full, pair], [own, far_first, near, *rest, resist, grad], work, held,
        in_specs=specs + [HBM, VMEM], out_specs=[HBM, VMEM], aliases={14: 0},
    )
    grad_after = permute(grad, down_pairs)
    grad_before_odd = permute(grad, near_pairs)
    (gradient,) = call(
        gradient_kernel,
        [full],
        [
            grad, grad_before_even, grad_before_odd, grad_after, slope,
            tables["back_rows"], *tables["forward"],
        ],
        6 * area * 2 * freq_cols,
        [pltpu.VMEM(full, F32), pltpu.SemaphoreType.DMA((QUARTERS,))],
        out_specs=[HBM],
    )
    return (resist, gradient)


def solution(mesh):
    in_specs = (P(("parts", "tiles"), None), P(("parts", "tiles"), None), P(), P())
    out_specs = (P(("parts", "tiles"), None), P(("parts", "tiles"), None))
    return jax.shard_map(shards, mesh=mesh, in_specs=in_specs, out_specs=out_specs, check_vma=False)
```

```python
import math

import jax
import jax.numpy as jnp
import numpy as np
from jax import lax
from jax.experimental import pallas as pl
from jax.experimental.pallas import tpu as pltpu
from jax.sharding import PartitionSpec as P


MARGIN = 64

STEEPNESS = 8.0
THRESHOLD = 0.35

BF16 = jnp.bfloat16
F32 = jnp.float32
QUARTERS = 4
GROUP = 8
LIMIT = 32 << 20


def split_table(table):
    table = np.asarray(table, np.float32)
    high = table.astype(BF16)
    low = (table - high.astype(np.float32)).astype(BF16)
    return high, low


def stack_left(table):
    high, low = split_table(table)
    return np.concatenate([high, high, low], axis=1)


def stack_both(table):
    high, low = split_table(table)
    return np.concatenate(
        [np.concatenate([high, high], axis=1), np.concatenate([low, 0 * low], axis=1)], axis=0
    )


def angles(frequencies, positions, period):
    cycles = np.remainder(frequencies[:, None] * positions[None, :], period)
    return cycles * (2.0 * math.pi / period)


def interpolation(fine, coarse, bound, period):
    count = len(coarse)
    distance = fine[:, None] - coarse[None, :]
    total = np.ones_like(distance, dtype=np.float64)
    for frequency in range(1, bound):
        total += 2.0 * np.cos(np.remainder(frequency * distance, period) * (2.0 * math.pi / period))
    return total / count


def make_tables(strip_rows, margin, columns, freq_rows, freq_cols):
    window = strip_rows + 2 * margin
    row_freq = np.arange(freq_rows, dtype=np.float64) - freq_rows // 2
    col_freq = np.arange(freq_cols, dtype=np.float64) - freq_cols // 2
    rows_c, cols_c = 2 * freq_rows, 2 * freq_cols
    own = np.arange(margin, margin + strip_rows, dtype=np.float64)
    wide = np.arange(columns, dtype=np.float64)
    samples_r = np.arange(rows_c, dtype=np.float64) * (window / rows_c)
    samples_c = np.arange(cols_c, dtype=np.float64) * (columns / cols_c)
    factor = 1.0 / math.sqrt(window * columns)
    col_angle = angles(col_freq, wide[: columns // QUARTERS], columns)
    forward = np.concatenate([np.cos(col_angle).T, -np.sin(col_angle).T], axis=1) * factor
    row_angle = angles(row_freq, own, window)
    cos_r, sin_r = np.cos(row_angle), np.sin(row_angle)
    half = strip_rows // 2
    none = np.zeros((freq_rows, half))
    first = np.concatenate([cos_r[:, :half], none, sin_r[:, :half], none], axis=1)
    second = np.concatenate([none, cos_r[:, half:], none, sin_r[:, half:]], axis=1)
    project = np.concatenate([first, second], axis=0)
    back_rows = np.concatenate([cos_r, sin_r], axis=0).T
    coarse_r = angles(row_freq, samples_r, window)
    cos_f, sin_f = np.cos(coarse_r).T, np.sin(coarse_r).T
    field_rows = np.concatenate(
        [np.concatenate([cos_f, -sin_f], axis=1), np.concatenate([sin_f, cos_f], axis=1)], axis=0
    )
    coarse_c = angles(col_freq, samples_c, columns)
    cos_c, sin_c = np.cos(coarse_c), np.sin(coarse_c)
    field_cols = np.concatenate(
        [np.concatenate([cos_c, sin_c], axis=1), np.concatenate([-sin_c, cos_c], axis=1)], axis=0
    )
    widen_rows = interpolation(own, samples_r, freq_rows, window)
    widen_cols = interpolation(wide, samples_c, freq_cols, columns).T
    return {
        "forward": split_table(forward),
        "project": split_table(project),
        "back_rows": stack_left(back_rows),
        "field_rows": stack_left(field_rows),
        "field_rows_t": stack_both(field_rows.T),
        "field_cols": split_table(field_cols),
        "widen_rows": stack_left(widen_rows),
        "widen_rows_t": stack_left(widen_rows.T),
        "widen_cols": split_table(widen_cols),
    }


def split(value):
    high = value.astype(BF16)
    return high, (value - high.astype(F32)).astype(BF16)


def stack_right(value):
    high, low = split(value)
    return jnp.concatenate([high, low, high], axis=0)


def stack_turned(pair):
    high, low = (turn(piece, 1) for piece in split(pair))
    return jnp.concatenate([high, low, high], axis=0)


def dot(left, right):
    return jnp.dot(left, right, preferred_element_type=F32)


def dot_t(left, right):
    return lax.dot_general(left, right, (((1,), (1,)), ((), ())), preferred_element_type=F32)


def dot3(left, right):
    (lh, ll), (rh, rl) = left, right
    return dot(lh, rh) + dot(lh, rl) + dot(ll, rh)


def dot3_t(left, right):
    (lh, ll), (rh, rl) = left, right
    return dot_t(lh, rh) + dot_t(lh, rl) + dot_t(ll, rh)


def turn(pair, sign):
    half = pair.shape[1] // 2
    real, imag = pair[:, :half], pair[:, half:]
    if sign > 0:
        turned = jnp.concatenate([-imag, real], axis=1)
    else:
        turned = jnp.concatenate([imag, -real], axis=1)
    return jnp.concatenate([pair, turned], axis=0)


def alternate(shape):
    row = lax.broadcasted_iota(jnp.int32, shape, 0)
    return jnp.where(row % 2 == 0, 1.0, -1.0).astype(F32)


def is_first():
    return lax.axis_index("tiles") == 0


def is_last():
    return lax.axis_index("tiles") == lax.axis_size("tiles") - 1


def is_odd():
    return lax.axis_index("tiles") % 2 == 1


def quarters(ref):
    width = ref.shape[1] // QUARTERS
    return [pl.ds(i * width, width) for i in range(QUARTERS)]


def quarter_turn(pair, count):
    half = pair.shape[1] // 2
    real, imag = pair[:, :half], pair[:, half:]
    lane = lax.broadcasted_iota(jnp.int32, (1, half), 1) - half // 2
    phase = (lane * count) & 3
    cosine = (phase == 0).astype(F32) - (phase == 2).astype(F32)
    sine = (phase == 1).astype(F32) - (phase == 3).astype(F32)
    return jnp.concatenate(
        [real * cosine - imag * sine, real * sine + imag * cosine], axis=1
    )


def project(
    mask_hbm, fwd_h_hbm, fwd_l_hbm, proj_h_hbm, proj_l_hbm, weights_hbm, slope_out, share_out, scratch
):
    mask, fwd_h, fwd_l, proj_h, proj_l, weights, sems = scratch
    columns = quarters(mask)
    masks = [pltpu.make_async_copy(mask_hbm, mask, sems.at[0, 0])]
    tables = [
        pltpu.make_async_copy(fwd_h_hbm, fwd_h, sems.at[1, 0]),
        pltpu.make_async_copy(fwd_l_hbm, fwd_l, sems.at[1, 1]),
    ]
    last = [
        pltpu.make_async_copy(weights_hbm, weights, sems.at[2, 2]),
        pltpu.make_async_copy(proj_h_hbm, proj_h, sems.at[2, 0]),
        pltpu.make_async_copy(proj_l_hbm, proj_l, sems.at[2, 1]),
    ]
    for copy in [*masks, *tables, *last]:
        copy.start()
    spectra = None
    for i, cols in enumerate(columns):
        if i == 0:
            last[0].wait()
            kernels, width = share_out.shape
            whole = weights[0]
            for k in range(1, kernels):
                whole = whole + weights[k]
            rows = [jnp.full((1, width), weights[k], F32) for k in range(kernels)]
            share_out[...] = jnp.concatenate(rows, axis=0) / jnp.full((kernels, width), whole, F32)
        if i == 0:
            masks[0].wait()
        transmit = jnp.tanh(mask[:, cols])
        slope_out[:, cols] = 1.0 - transmit * transmit
        pieces = split(transmit)
        if i == 0:
            for copy in tables:
                copy.wait()
        term = quarter_turn(dot3(pieces, (fwd_h[...], fwd_l[...])), -i)
        spectra = term if spectra is None else spectra + term
    for copy in last[1:]:
        copy.wait()
    parts = dot3((proj_h[...], proj_l[...]), split(turn(spectra, -1)))
    half = parts.shape[0] // 2
    return parts[:half], parts[half:]


def project_first(*refs):
    args, (far, near, own, share, slope), scratch = refs[:6], refs[6:11], refs[11:]

    @pl.when(jnp.logical_not(is_last()))
    def _():
        low, high = project(*args, slope, share, scratch)
        odd = is_odd()
        far[...] = jnp.where(odd, high, low)
        near[...] = jnp.where(odd, low, high)
        own[...] = low + high


def project_second(*refs):
    args, taken, refs = refs[:6], refs[6:10], refs[11:]
    (far, near, own, share, slope), scratch = refs[:5], refs[5:]

    @pl.when(is_last())
    def _():
        low, high = project(*args, slope, share, scratch)
        far[...], near[...], own[...] = high, low, low + high

    @pl.when(jnp.logical_not(is_last()))
    def _():
        far[...], near[...], own[...], share[...] = (ref[...] for ref in taken)


def image(
    own, far, near, spectra, shares, target, rows_f, rows_t, cols_h, cols_l,
    wide_r, wide_rt, wide_h, wide_l, resist_hbm, grad_out, fields, resist_out, sem
):
    kernels, freq_rows, freq_cols = spectra.shape[1:]
    rows_c, cols_c = rows_f.shape[0] // 2, 2 * freq_cols
    group = math.gcd(kernels, GROUP)
    sign = alternate(own.shape)
    window = own[...] + sign * (far[...] + near[...])
    win_re, win_im = window[:, :freq_cols], window[:, freq_cols:]

    def forward(step, total):
        start = step * group
        prods = []
        for j in range(group):
            kern_re, kern_im = spectra[0, start + j], spectra[1, start + j]
            prods.append(jnp.concatenate(
                [kern_re * win_re - kern_im * win_im, kern_re * win_im + kern_im * win_re], axis=1
            ))
        inner = dot3(split(jnp.concatenate(prods, axis=0)), (cols_h[...], cols_l[...]))
        for j in range(group):
            part = inner[j * freq_rows : (j + 1) * freq_rows]
            part = jnp.concatenate([part[:, :cols_c], part[:, cols_c:]], axis=0)
            field = dot(rows_f[...], stack_right(part))
            fields[start + j] = field
            power = field[:rows_c] ** 2 + field[rows_c:] ** 2
            total = total + shares[pl.ds(start + j, 1), :] * power
        return total

    total = lax.fori_loop(0, kernels // group, forward, jnp.zeros((rows_c, cols_c), F32))
    tall = dot(wide_r[...], stack_right(total))
    intensity = dot3(split(tall), (wide_h[...], wide_l[...]))
    resist = jax.nn.sigmoid(STEEPNESS * (intensity - THRESHOLD))
    resist_out[...] = resist
    sent = pltpu.make_async_copy(resist_out, resist_hbm, sem)
    sent.start()
    slopes = (4.0 * STEEPNESS) * (resist - target[...].astype(F32)) * resist * (1.0 - resist)
    narrow = dot3_t(split(slopes), (wide_h[...], wide_l[...]))
    weight = dot(wide_rt[...], stack_right(narrow))
    weight = jnp.concatenate([weight, weight], axis=0)

    def backward(step, sums):
        grad_re, grad_im = sums
        start = step * group
        inners = []
        for j in range(group):
            pieces = jnp.concatenate(split(weight * fields[start + j]), axis=0)
            part = dot(rows_t[...], pieces)
            part = part[: 2 * freq_rows] + part[2 * freq_rows :]
            inners.append(jnp.concatenate([part[:freq_rows], part[freq_rows:]], axis=1))
        spec = dot3_t(split(jnp.concatenate(inners, axis=0)), (cols_h[...], cols_l[...]))
        for j in range(group):
            part = shares[pl.ds(start + j, 1), :] * spec[j * freq_rows : (j + 1) * freq_rows]
            real, imag = part[:, :freq_cols], part[:, freq_cols:]
            kern_re, kern_im = spectra[0, start + j], spectra[1, start + j]
            grad_re = grad_re + real * kern_re + imag * kern_im
            grad_im = grad_im + imag * kern_re - real * kern_im
        return grad_re, grad_im

    none = jnp.zeros((freq_rows, freq_cols), F32)
    grad_re, grad_im = lax.fori_loop(0, kernels // group, backward, (none, none))
    grad_out[...] = jnp.concatenate([grad_re, grad_im], axis=1)
    sent.wait()


def image_first(*refs):
    @pl.when(jnp.logical_not(is_first()))
    def _():
        image(*refs)


def image_second(*refs):
    args, (_, grad_in), refs = refs[:14], refs[14:16], refs[16:]

    @pl.when(is_first())
    def _():
        image(*args, *refs)

    @pl.when(jnp.logical_not(is_first()))
    def _():
        refs[1][...] = grad_in[...]


def gradient(own, before, after, slope, rows_b, fwd_h, fwd_l, out_hbm, out, sems):
    half = out.shape[0] // 2
    sign = alternate(own.shape)
    low = stack_turned(own[...] + sign * before)
    high = stack_turned(own[...] + sign * after)
    merged = jnp.concatenate([dot(rows_b[:half], low), dot(rows_b[half:], high)], axis=0)
    sent = []
    for i, cols in enumerate(quarters(out)):
        pieces = split(quarter_turn(merged, i))
        out[:, cols] = slope[:, cols] * dot3_t(pieces, (fwd_h[...], fwd_l[...]))
        sent.append(pltpu.make_async_copy(out.at[:, cols], out_hbm.at[:, cols], sems.at[i]))
        sent[-1].start()
    for copy in sent:
        copy.wait()


def gradient_first(own, before, after, *refs):
    @pl.when(is_first())
    def _():
        gradient(own, before[...], after[...], *refs)


def gradient_second(own, before_even, before_odd, after, slope, rows_b, fwd_h, fwd_l, _, *refs):
    @pl.when(jnp.logical_not(is_first()))
    def _():
        before = jnp.where(is_odd(), before_odd[...], before_even[...])
        gradient(own, before, after[...], slope, rows_b, fwd_h, fwd_l, *refs)


VMEM = pl.BlockSpec(memory_space=pltpu.VMEM)
HBM = pl.BlockSpec(memory_space=pltpu.HBM)


def call(kernel, outs, args, flops, scratch, out_specs, in_specs=None, aliases=None):
    shapes = [jax.ShapeDtypeStruct(shape, F32) for shape in outs]
    moved = sum(math.prod(a.shape) * a.dtype.itemsize for a in args)
    moved += sum(4 * math.prod(shape) for shape in outs)
    return pl.pallas_call(
        kernel,
        out_shape=shapes,
        in_specs=in_specs or [VMEM] * len(args),
        out_specs=out_specs,
        scratch_shapes=scratch,
        input_output_aliases=aliases or {},
        compiler_params=pltpu.CompilerParams(vmem_limit_bytes=LIMIT),
        cost_estimate=pl.CostEstimate(flops=flops, bytes_accessed=moved, transcendentals=0),
    )(*args)


def permute(value, pairs):
    return lax.ppermute(value, "tiles", pairs)


def shards(mask_params, target, kernel_spectra, kernel_weights):
    strip_rows, columns = mask_params.shape
    kernels, freq_rows, freq_cols = kernel_spectra.shape[1:]
    tables = jax.tree.map(
        jnp.asarray, make_tables(strip_rows, MARGIN, columns, freq_rows, freq_cols)
    )
    count = lax.axis_size("tiles")
    assert 2 * MARGIN == strip_rows and count % 2 == 0 and count >= 6
    near_pairs = [(i, i ^ 1) for i in range(count)]
    far_pairs = [(i, (i + 1 if i % 2 else i - 1) % count) for i in range(count)]
    last = count - 1
    ends = [(last, 0), (0, last - 1), (last - 1, last), (1, 2), (2, 3), (3, 1)]
    wrap1_pairs = ends + near_pairs[4 : last - 1]
    up_pairs = [(i, (i + 1) % count) for i in range(count)]
    down_pairs = [(j, i) for i, j in up_pairs]
    pair, full, wide = (freq_rows, 2 * freq_cols), (strip_rows, columns), (kernels, 2 * freq_cols)
    area = strip_rows * columns

    args = [mask_params, *tables["forward"], *tables["project"]]
    held = [pltpu.VMEM(a.shape, a.dtype) for a in args]
    held += [pltpu.SMEM((kernels,), F32), pltpu.SemaphoreType.DMA((3, QUARTERS))]
    args.append(kernel_weights)
    args = [pltpu.with_memory_space_constraint(a, pltpu.HBM) for a in args]
    work = 60 * area * 2 * freq_cols
    send_far, send_near, own, share, slope = call(
        project_first, [pair, pair, pair, wide, full], args, work, held,
        in_specs=[HBM] * 6, out_specs=[VMEM] * 5,
    )
    far = permute(send_far, far_pairs)
    send_far, send_near, own, share, slope = call(
        project_second, [pair, pair, pair, wide, full],
        [*args, send_far, send_near, own, share, slope],
        work, held, in_specs=[HBM] * 6 + [VMEM] * 5, out_specs=[VMEM] * 5, aliases={10: 4},
    )
    near = permute(send_near, near_pairs)
    far_first = permute(send_far, wrap1_pairs)

    rows_c, cols_c = 2 * freq_rows, 2 * freq_cols
    held = [
        pltpu.VMEM((kernels, 2 * rows_c, cols_c), F32),
        pltpu.VMEM(full, F32),
        pltpu.SemaphoreType.DMA,
    ]
    rest = [
        kernel_spectra, share, target,
        tables["field_rows"], tables["field_rows_t"], *tables["field_cols"],
        tables["widen_rows"], tables["widen_rows_t"], *tables["widen_cols"],
    ]
    specs = [VMEM] * 14
    work = 24 * kernels * rows_c * cols_c * cols_c
    resist, grad = call(
        image_first, [full, pair], [own, far, near, *rest], work, held,
        in_specs=specs, out_specs=[HBM, VMEM],
    )
    grad_after_first = permute(grad, near_pairs)
    grad_before_even = permute(grad, up_pairs)
    resist, grad = call(
        image_second, [full, pair], [own, far_first, near, *rest, resist, grad], work, held,
        in_specs=specs + [HBM, VMEM], out_specs=[HBM, VMEM], aliases={14: 0},
    )
    grad_after = permute(grad, down_pairs)
    grad_before_odd = permute(grad, near_pairs)
    rest = [slope, tables["back_rows"], *tables["forward"]]
    held = [pltpu.VMEM(full, F32), pltpu.SemaphoreType.DMA((QUARTERS,))]
    work = 6 * area * 2 * freq_cols
    (gradient,) = call(
        gradient_first, [full], [grad, grad_before_even, grad_after_first, *rest], work, held,
        out_specs=[HBM],
    )
    (gradient,) = call(
        gradient_second, [full],
        [grad, grad_before_even, grad_before_odd, grad_after, *rest, gradient], work, held,
        in_specs=[VMEM] * 8 + [HBM], out_specs=[HBM], aliases={8: 0},
    )
    return (resist, gradient)


def solution(mesh):
    in_specs = (P(("parts", "tiles"), None), P(("parts", "tiles"), None), P(), P())
    out_specs = (P(("parts", "tiles"), None), P(("parts", "tiles"), None))
    return jax.shard_map(shards, mesh=mesh, in_specs=in_specs, out_specs=out_specs, check_vma=False)
```

```python
import math

import jax
import jax.numpy as jnp
import numpy as np
from jax import lax
from jax.experimental import pallas as pl
from jax.experimental.pallas import tpu as pltpu
from jax.sharding import PartitionSpec as P


MARGIN = 64

STEEPNESS = 8.0
THRESHOLD = 0.35

BF16 = jnp.bfloat16
F32 = jnp.float32
QUARTERS = 4
GROUP = 8
LIMIT = 32 << 20


def split_table(table):
    table = np.asarray(table, np.float32)
    high = table.astype(BF16)
    low = (table - high.astype(np.float32)).astype(BF16)
    return high, low


def stack_left(table):
    high, low = split_table(table)
    return np.concatenate([high, high, low], axis=1)


def stack_both(table):
    high, low = split_table(table)
    return np.concatenate(
        [np.concatenate([high, high], axis=1), np.concatenate([low, 0 * low], axis=1)], axis=0
    )


def angles(frequencies, positions, period):
    cycles = np.remainder(frequencies[:, None] * positions[None, :], period)
    return cycles * (2.0 * math.pi / period)


def interpolation(fine, coarse, bound, period):
    count = len(coarse)
    distance = fine[:, None] - coarse[None, :]
    total = np.ones_like(distance, dtype=np.float64)
    for frequency in range(1, bound):
        total += 2.0 * np.cos(np.remainder(frequency * distance, period) * (2.0 * math.pi / period))
    return total / count


def make_tables(strip_rows, margin, columns, freq_rows, freq_cols):
    window = strip_rows + 2 * margin
    row_freq = np.arange(freq_rows, dtype=np.float64) - freq_rows // 2
    col_freq = np.arange(freq_cols, dtype=np.float64) - freq_cols // 2
    rows_c, cols_c = 2 * freq_rows, 2 * freq_cols
    own = np.arange(margin, margin + strip_rows, dtype=np.float64)
    wide = np.arange(columns, dtype=np.float64)
    samples_r = np.arange(rows_c, dtype=np.float64) * (window / rows_c)
    samples_c = np.arange(cols_c, dtype=np.float64) * (columns / cols_c)
    factor = 1.0 / math.sqrt(window * columns)
    col_angle = angles(col_freq, wide[: columns // QUARTERS], columns)
    forward = np.concatenate([np.cos(col_angle).T, -np.sin(col_angle).T], axis=1) * factor
    row_angle = angles(row_freq, own, window)
    cos_r, sin_r = np.cos(row_angle), np.sin(row_angle)
    half = strip_rows // 2
    none = np.zeros((freq_rows, half))
    first = np.concatenate([cos_r[:, :half], none, sin_r[:, :half], none], axis=1)
    second = np.concatenate([none, cos_r[:, half:], none, sin_r[:, half:]], axis=1)
    project = np.concatenate([first, second], axis=0)
    back_rows = np.concatenate([cos_r, sin_r], axis=0).T
    coarse_r = angles(row_freq, samples_r, window)
    cos_f, sin_f = np.cos(coarse_r).T, np.sin(coarse_r).T
    field_rows = np.concatenate(
        [np.concatenate([cos_f, -sin_f], axis=1), np.concatenate([sin_f, cos_f], axis=1)], axis=0
    )
    coarse_c = angles(col_freq, samples_c, columns)
    cos_c, sin_c = np.cos(coarse_c), np.sin(coarse_c)
    field_cols = np.concatenate(
        [np.concatenate([cos_c, sin_c], axis=1), np.concatenate([-sin_c, cos_c], axis=1)], axis=0
    )
    widen_rows = interpolation(own, samples_r, freq_rows, window)
    widen_cols = interpolation(wide, samples_c, freq_cols, columns).T
    return {
        "forward": split_table(forward),
        "project": split_table(project),
        "back_rows": stack_left(back_rows),
        "field_rows": stack_left(field_rows),
        "field_rows_t": stack_both(field_rows.T),
        "field_cols": split_table(field_cols),
        "widen_rows": stack_left(widen_rows),
        "widen_rows_t": stack_left(widen_rows.T),
        "widen_cols": split_table(widen_cols),
    }


def split(value):
    high = value.astype(BF16)
    return high, (value - high.astype(F32)).astype(BF16)


def stack_right(value):
    high, low = split(value)
    return jnp.concatenate([high, low, high], axis=0)


def stack_turned(pair):
    high, low = (turn(piece, 1) for piece in split(pair))
    return jnp.concatenate([high, low, high], axis=0)


def dot(left, right):
    return jnp.dot(left, right, preferred_element_type=F32)


def dot_t(left, right):
    return lax.dot_general(left, right, (((1,), (1,)), ((), ())), preferred_element_type=F32)


def dot3(left, right):
    (lh, ll), (rh, rl) = left, right
    return dot(lh, rh) + dot(lh, rl) + dot(ll, rh)


def dot3_t(left, right):
    (lh, ll), (rh, rl) = left, right
    return dot_t(lh, rh) + dot_t(lh, rl) + dot_t(ll, rh)


def turn(pair, sign):
    half = pair.shape[1] // 2
    real, imag = pair[:, :half], pair[:, half:]
    if sign > 0:
        turned = jnp.concatenate([-imag, real], axis=1)
    else:
        turned = jnp.concatenate([imag, -real], axis=1)
    return jnp.concatenate([pair, turned], axis=0)


def alternate(shape):
    row = lax.broadcasted_iota(jnp.int32, shape, 0)
    return jnp.where(row % 2 == 0, 1.0, -1.0).astype(F32)


def is_first():
    return lax.axis_index("tiles") == 0


def is_last():
    return lax.axis_index("tiles") == lax.axis_size("tiles") - 1


def is_odd():
    return lax.axis_index("tiles") % 2 == 1


def quarters(ref):
    width = ref.shape[1] // QUARTERS
    return [pl.ds(i * width, width) for i in range(QUARTERS)]


def quarter_turn(pair, count):
    half = pair.shape[1] // 2
    real, imag = pair[:, :half], pair[:, half:]
    lane = lax.broadcasted_iota(jnp.int32, (1, half), 1) - half // 2
    phase = (lane * count) & 3
    cosine = (phase == 0).astype(F32) - (phase == 2).astype(F32)
    sine = (phase == 1).astype(F32) - (phase == 3).astype(F32)
    return jnp.concatenate(
        [real * cosine - imag * sine, real * sine + imag * cosine], axis=1
    )


def project(
    mask_hbm, fwd_h_hbm, fwd_l_hbm, proj_h_hbm, proj_l_hbm, weights_hbm, slope_out, share_out, scratch
):
    mask, fwd_h, fwd_l, proj_h, proj_l, weights, sems = scratch
    columns = quarters(mask)
    masks = [pltpu.make_async_copy(mask_hbm, mask, sems.at[0, 0])]
    tables = [
        pltpu.make_async_copy(fwd_h_hbm, fwd_h, sems.at[1, 0]),
        pltpu.make_async_copy(fwd_l_hbm, fwd_l, sems.at[1, 1]),
    ]
    last = [
        pltpu.make_async_copy(weights_hbm, weights, sems.at[2, 2]),
        pltpu.make_async_copy(proj_h_hbm, proj_h, sems.at[2, 0]),
        pltpu.make_async_copy(proj_l_hbm, proj_l, sems.at[2, 1]),
    ]
    for copy in [*masks, *tables, *last]:
        copy.start()
    spectra = None
    for i, cols in enumerate(columns):
        if i == 0:
            last[0].wait()
            kernels, width = share_out.shape
            whole = weights[0]
            for k in range(1, kernels):
                whole = whole + weights[k]
            rows = [jnp.full((1, width), weights[k], F32) for k in range(kernels)]
            share_out[...] = jnp.concatenate(rows, axis=0) / jnp.full((kernels, width), whole, F32)
        if i == 0:
            masks[0].wait()
        transmit = jnp.tanh(mask[:, cols])
        slope_out[:, cols] = 1.0 - transmit * transmit
        pieces = split(transmit)
        if i == 0:
            for copy in tables:
                copy.wait()
        term = quarter_turn(dot3(pieces, (fwd_h[...], fwd_l[...])), -i)
        spectra = term if spectra is None else spectra + term
    for copy in last[1:]:
        copy.wait()
    parts = dot3((proj_h[...], proj_l[...]), split(turn(spectra, -1)))
    half = parts.shape[0] // 2
    return parts[:half], parts[half:]


def project_first(*refs):
    args, (far, near, own, share, slope), scratch = refs[:6], refs[6:11], refs[11:]

    @pl.when(jnp.logical_not(is_last()))
    def _():
        low, high = project(*args, slope, share, scratch)
        odd = is_odd()
        far[...] = jnp.where(odd, high, low)
        near[...] = jnp.where(odd, low, high)
        own[...] = low + high


def project_second(*refs):
    args, taken, refs = refs[:6], refs[6:10], refs[11:]
    (far, near, own, share, slope), scratch = refs[:5], refs[5:]

    @pl.when(is_last())
    def _():
        low, high = project(*args, slope, share, scratch)
        far[...], near[...], own[...] = high, low, low + high

    @pl.when(jnp.logical_not(is_last()))
    def _():
        far[...], near[...], own[...], share[...] = (ref[...] for ref in taken)


def image(
    own, far, near, spectra, shares, target, rows_f, rows_t, cols_h, cols_l,
    wide_r, wide_rt, wide_h, wide_l, resist_hbm, grad_out, fields, resist_out, sem
):
    kernels, freq_rows, freq_cols = spectra.shape[1:]
    rows_c, cols_c = rows_f.shape[0] // 2, 2 * freq_cols
    group = math.gcd(kernels, GROUP)
    sign = alternate(own.shape)
    window = own[...] + sign * (far[...] + near[...])
    win_re, win_im = window[:, :freq_cols], window[:, freq_cols:]

    def forward(step, total):
        start = step * group
        prods = []
        for j in range(group):
            kern_re, kern_im = spectra[0, start + j], spectra[1, start + j]
            prods.append(jnp.concatenate(
                [kern_re * win_re - kern_im * win_im, kern_re * win_im + kern_im * win_re], axis=1
            ))
        inner = dot3(split(jnp.concatenate(prods, axis=0)), (cols_h[...], cols_l[...]))
        for j in range(group):
            part = inner[j * freq_rows : (j + 1) * freq_rows]
            part = jnp.concatenate([part[:, :cols_c], part[:, cols_c:]], axis=0)
            field = dot(rows_f[...], stack_right(part))
            fields[start + j] = field
            power = field[:rows_c] ** 2 + field[rows_c:] ** 2
            total = total + shares[pl.ds(start + j, 1), :] * power
        return total

    total = lax.fori_loop(0, kernels // group, forward, jnp.zeros((rows_c, cols_c), F32))
    tall = dot(wide_r[...], stack_right(total))
    intensity = dot3(split(tall), (wide_h[...], wide_l[...]))
    resist = jax.nn.sigmoid(STEEPNESS * (intensity - THRESHOLD))
    resist_out[...] = resist
    sent = pltpu.make_async_copy(resist_out, resist_hbm, sem)
    sent.start()
    slopes = (4.0 * STEEPNESS) * (resist - target[...].astype(F32)) * resist * (1.0 - resist)
    narrow = dot3_t(split(slopes), (wide_h[...], wide_l[...]))
    weight = dot(wide_rt[...], stack_right(narrow))
    weight = jnp.concatenate([weight, weight], axis=0)

    def backward(step, sums):
        grad_re, grad_im = sums
        start = step * group
        inners = []
        for j in range(group):
            pieces = jnp.concatenate(split(weight * fields[start + j]), axis=0)
            part = dot(rows_t[...], pieces)
            part = part[: 2 * freq_rows] + part[2 * freq_rows :]
            inners.append(jnp.concatenate([part[:freq_rows], part[freq_rows:]], axis=1))
        spec = dot3_t(split(jnp.concatenate(inners, axis=0)), (cols_h[...], cols_l[...]))
        for j in range(group):
            part = shares[pl.ds(start + j, 1), :] * spec[j * freq_rows : (j + 1) * freq_rows]
            real, imag = part[:, :freq_cols], part[:, freq_cols:]
            kern_re, kern_im = spectra[0, start + j], spectra[1, start + j]
            grad_re = grad_re + real * kern_re + imag * kern_im
            grad_im = grad_im + imag * kern_re - real * kern_im
        return grad_re, grad_im

    none = jnp.zeros((freq_rows, freq_cols), F32)
    grad_re, grad_im = lax.fori_loop(0, kernels // group, backward, (none, none))
    grad_out[...] = jnp.concatenate([grad_re, grad_im], axis=1)
    sent.wait()


def image_first(*refs):
    @pl.when(jnp.logical_not(is_first()))
    def _():
        image(*refs)


def image_second(*refs):
    args, (_, grad_in), refs = refs[:14], refs[14:16], refs[16:]

    @pl.when(is_first())
    def _():
        image(*args, *refs)

    @pl.when(jnp.logical_not(is_first()))
    def _():
        refs[1][...] = grad_in[...]


def gradient(own, before, after, slope, rows_b, fwd_h, fwd_l, out_hbm, out, sems):
    half = out.shape[0] // 2
    sign = alternate(own.shape)
    low = stack_turned(own[...] + sign * before)
    high = stack_turned(own[...] + sign * after)
    merged = jnp.concatenate([dot(rows_b[:half], low), dot(rows_b[half:], high)], axis=0)
    parts = [quarter_turn(merged, i) for i in range(QUARTERS)]
    pieces = split(jnp.concatenate(parts, axis=0))
    terms = dot3_t(pieces, (fwd_h[...], fwd_l[...]))
    rows = out.shape[0]
    for i, cols in enumerate(quarters(out)):
        out[:, cols] = slope[:, cols] * terms[i * rows : (i + 1) * rows]
    sent = pltpu.make_async_copy(out, out_hbm, sems.at[0])
    sent.start()
    sent.wait()


def gradient_first(own, before, after, *refs):
    @pl.when(is_first())
    def _():
        gradient(own, before[...], after[...], *refs)


def gradient_second(own, before_even, before_odd, after, slope, rows_b, fwd_h, fwd_l, _, *refs):
    @pl.when(jnp.logical_not(is_first()))
    def _():
        before = jnp.where(is_odd(), before_odd[...], before_even[...])
        gradient(own, before, after[...], slope, rows_b, fwd_h, fwd_l, *refs)


VMEM = pl.BlockSpec(memory_space=pltpu.VMEM)
HBM = pl.BlockSpec(memory_space=pltpu.HBM)


def call(kernel, outs, args, flops, scratch, out_specs, in_specs=None, aliases=None):
    shapes = [jax.ShapeDtypeStruct(shape, F32) for shape in outs]
    moved = sum(math.prod(a.shape) * a.dtype.itemsize for a in args)
    moved += sum(4 * math.prod(shape) for shape in outs)
    return pl.pallas_call(
        kernel,
        out_shape=shapes,
        in_specs=in_specs or [VMEM] * len(args),
        out_specs=out_specs,
        scratch_shapes=scratch,
        input_output_aliases=aliases or {},
        compiler_params=pltpu.CompilerParams(vmem_limit_bytes=LIMIT),
        cost_estimate=pl.CostEstimate(flops=flops, bytes_accessed=moved, transcendentals=0),
    )(*args)


def permute(value, pairs):
    return lax.ppermute(value, "tiles", pairs)


def shards(mask_params, target, kernel_spectra, kernel_weights):
    strip_rows, columns = mask_params.shape
    kernels, freq_rows, freq_cols = kernel_spectra.shape[1:]
    tables = jax.tree.map(
        jnp.asarray, make_tables(strip_rows, MARGIN, columns, freq_rows, freq_cols)
    )
    count = lax.axis_size("tiles")
    assert 2 * MARGIN == strip_rows and count % 2 == 0 and count >= 6
    near_pairs = [(i, i ^ 1) for i in range(count)]
    far_pairs = [(i, (i + 1 if i % 2 else i - 1) % count) for i in range(count)]
    last = count - 1
    ends = [(last, 0), (0, last - 1), (last - 1, last), (1, 2), (2, 3), (3, 1)]
    wrap1_pairs = ends + near_pairs[4 : last - 1]
    up_pairs = [(i, (i + 1) % count) for i in range(count)]
    down_pairs = [(j, i) for i, j in up_pairs]
    pair, full, wide = (freq_rows, 2 * freq_cols), (strip_rows, columns), (kernels, 2 * freq_cols)
    area = strip_rows * columns

    args = [mask_params, *tables["forward"], *tables["project"]]
    held = [pltpu.VMEM(a.shape, a.dtype) for a in args]
    held += [pltpu.SMEM((kernels,), F32), pltpu.SemaphoreType.DMA((3, QUARTERS))]
    args.append(kernel_weights)
    args = [pltpu.with_memory_space_constraint(a, pltpu.HBM) for a in args]
    work = 60 * area * 2 * freq_cols
    send_far, send_near, own, share, slope = call(
        project_first, [pair, pair, pair, wide, full], args, work, held,
        in_specs=[HBM] * 6, out_specs=[VMEM] * 5,
    )
    far = permute(send_far, far_pairs)
    send_far, send_near, own, share, slope = call(
        project_second, [pair, pair, pair, wide, full],
        [*args, send_far, send_near, own, share, slope],
        work, held, in_specs=[HBM] * 6 + [VMEM] * 5, out_specs=[VMEM] * 5, aliases={10: 4},
    )
    near = permute(send_near, near_pairs)
    far_first = permute(send_far, wrap1_pairs)

    rows_c, cols_c = 2 * freq_rows, 2 * freq_cols
    held = [
        pltpu.VMEM((kernels, 2 * rows_c, cols_c), F32),
        pltpu.VMEM(full, F32),
        pltpu.SemaphoreType.DMA,
    ]
    rest = [
        kernel_spectra, share, target,
        tables["field_rows"], tables["field_rows_t"], *tables["field_cols"],
        tables["widen_rows"], tables["widen_rows_t"], *tables["widen_cols"],
    ]
    specs = [VMEM] * 14
    work = 24 * kernels * rows_c * cols_c * cols_c
    resist, grad = call(
        image_first, [full, pair], [own, far, near, *rest], work, held,
        in_specs=specs, out_specs=[HBM, VMEM],
    )
    grad_after_first = permute(grad, near_pairs)
    grad_before_even = permute(grad, up_pairs)
    resist, grad = call(
        image_second, [full, pair], [own, far_first, near, *rest, resist, grad], work, held,
        in_specs=specs + [HBM, VMEM], out_specs=[HBM, VMEM], aliases={14: 0},
    )
    grad_after = permute(grad, down_pairs)
    grad_before_odd = permute(grad, near_pairs)
    rest = [slope, tables["back_rows"], *tables["forward"]]
    held = [pltpu.VMEM(full, F32), pltpu.SemaphoreType.DMA((QUARTERS,))]
    work = 6 * area * 2 * freq_cols
    (gradient,) = call(
        gradient_first, [full], [grad, grad_before_even, grad_after_first, *rest], work, held,
        out_specs=[HBM],
    )
    (gradient,) = call(
        gradient_second, [full],
        [grad, grad_before_even, grad_before_odd, grad_after, *rest, gradient], work, held,
        in_specs=[VMEM] * 8 + [HBM], out_specs=[HBM], aliases={8: 0},
    )
    return (resist, gradient)


def solution(mesh):
    in_specs = (P(("parts", "tiles"), None), P(("parts", "tiles"), None), P(), P())
    out_specs = (P(("parts", "tiles"), None), P(("parts", "tiles"), None))
    return jax.shard_map(shards, mesh=mesh, in_specs=in_specs, out_specs=out_specs, check_vma=False)
```

```python
import math

import jax
import jax.numpy as jnp
import numpy as np
from jax import lax
from jax.experimental import pallas as pl
from jax.experimental.pallas import tpu as pltpu
from jax.sharding import PartitionSpec as P


MARGIN = 64

STEEPNESS = 8.0
THRESHOLD = 0.35

BF16 = jnp.bfloat16
F32 = jnp.float32
QUARTERS = 4
GROUP = 8
LIMIT = 32 << 20


def split_table(table):
    table = np.asarray(table, np.float32)
    high = table.astype(BF16)
    low = (table - high.astype(np.float32)).astype(BF16)
    return high, low


def stack_left(table):
    high, low = split_table(table)
    return np.concatenate([high, high, low], axis=1)


def stack_both(table):
    high, low = split_table(table)
    return np.concatenate(
        [np.concatenate([high, high], axis=1), np.concatenate([low, 0 * low], axis=1)], axis=0
    )


def angles(frequencies, positions, period):
    cycles = np.remainder(frequencies[:, None] * positions[None, :], period)
    return cycles * (2.0 * math.pi / period)


def interpolation(fine, coarse, bound, period):
    count = len(coarse)
    distance = fine[:, None] - coarse[None, :]
    total = np.ones_like(distance, dtype=np.float64)
    for frequency in range(1, bound):
        total += 2.0 * np.cos(np.remainder(frequency * distance, period) * (2.0 * math.pi / period))
    return total / count


def make_tables(strip_rows, margin, columns, freq_rows, freq_cols):
    window = strip_rows + 2 * margin
    row_freq = np.arange(freq_rows, dtype=np.float64) - freq_rows // 2
    col_freq = np.arange(freq_cols, dtype=np.float64) - freq_cols // 2
    rows_c, cols_c = 2 * freq_rows, 2 * freq_cols
    own = np.arange(margin, margin + strip_rows, dtype=np.float64)
    wide = np.arange(columns, dtype=np.float64)
    samples_r = np.arange(rows_c, dtype=np.float64) * (window / rows_c)
    samples_c = np.arange(cols_c, dtype=np.float64) * (columns / cols_c)
    factor = 1.0 / math.sqrt(window * columns)
    col_angle = angles(col_freq, wide[: columns // QUARTERS], columns)
    forward = np.concatenate([np.cos(col_angle).T, -np.sin(col_angle).T], axis=1) * factor
    row_angle = angles(row_freq, own, window)
    cos_r, sin_r = np.cos(row_angle), np.sin(row_angle)
    half = strip_rows // 2
    none = np.zeros((freq_rows, half))
    first = np.concatenate([cos_r[:, :half], none, sin_r[:, :half], none], axis=1)
    second = np.concatenate([none, cos_r[:, half:], none, sin_r[:, half:]], axis=1)
    project = np.concatenate([first, second], axis=0)
    back_rows = np.concatenate([cos_r, sin_r], axis=0).T
    coarse_r = angles(row_freq, samples_r, window)
    cos_f, sin_f = np.cos(coarse_r).T, np.sin(coarse_r).T
    field_rows = np.concatenate(
        [np.concatenate([cos_f, -sin_f], axis=1), np.concatenate([sin_f, cos_f], axis=1)], axis=0
    )
    coarse_c = angles(col_freq, samples_c, columns)
    cos_c, sin_c = np.cos(coarse_c), np.sin(coarse_c)
    field_cols = np.concatenate(
        [np.concatenate([cos_c, sin_c], axis=1), np.concatenate([-sin_c, cos_c], axis=1)], axis=0
    )
    widen_rows = interpolation(own, samples_r, freq_rows, window)
    widen_cols = interpolation(wide, samples_c, freq_cols, columns).T
    return {
        "forward": split_table(forward),
        "project": split_table(project),
        "back_rows": stack_left(back_rows),
        "field_rows": stack_left(field_rows),
        "field_rows_t": stack_both(field_rows.T),
        "field_cols": split_table(field_cols),
        "widen_rows": stack_left(widen_rows),
        "widen_rows_t": stack_left(widen_rows.T),
        "widen_cols": split_table(widen_cols),
    }


def split(value):
    high = value.astype(BF16)
    return high, (value - high.astype(F32)).astype(BF16)


def stack_right(value):
    high, low = split(value)
    return jnp.concatenate([high, low, high], axis=0)


def stack_turned(pair):
    high, low = (turn(piece, 1) for piece in split(pair))
    return jnp.concatenate([high, low, high], axis=0)


def dot(left, right):
    return jnp.dot(left, right, preferred_element_type=F32)


def dot_t(left, right):
    return lax.dot_general(left, right, (((1,), (1,)), ((), ())), preferred_element_type=F32)


def dot3(left, right):
    (lh, ll), (rh, rl) = left, right
    return dot(lh, rh) + dot(lh, rl) + dot(ll, rh)


def dot3_t(left, right):
    (lh, ll), (rh, rl) = left, right
    return dot_t(lh, rh) + dot_t(lh, rl) + dot_t(ll, rh)


def turn(pair, sign):
    half = pair.shape[1] // 2
    real, imag = pair[:, :half], pair[:, half:]
    if sign > 0:
        turned = jnp.concatenate([-imag, real], axis=1)
    else:
        turned = jnp.concatenate([imag, -real], axis=1)
    return jnp.concatenate([pair, turned], axis=0)


def alternate(shape):
    row = lax.broadcasted_iota(jnp.int32, shape, 0)
    return jnp.where(row % 2 == 0, 1.0, -1.0).astype(F32)


def is_first():
    return lax.axis_index("tiles") == 0


def is_last():
    return lax.axis_index("tiles") == lax.axis_size("tiles") - 1


def is_odd():
    return lax.axis_index("tiles") % 2 == 1


def quarters(ref):
    width = ref.shape[1] // QUARTERS
    return [pl.ds(i * width, width) for i in range(QUARTERS)]


def quarter_turn(pair, count):
    half = pair.shape[1] // 2
    real, imag = pair[:, :half], pair[:, half:]
    lane = lax.broadcasted_iota(jnp.int32, (1, half), 1) - half // 2
    phase = (lane * count) & 3
    cosine = (phase == 0).astype(F32) - (phase == 2).astype(F32)
    sine = (phase == 1).astype(F32) - (phase == 3).astype(F32)
    return jnp.concatenate(
        [real * cosine - imag * sine, real * sine + imag * cosine], axis=1
    )


def project(
    mask_hbm, fwd_h_hbm, fwd_l_hbm, proj_h_hbm, proj_l_hbm, weights_hbm, slope_out, share_out, scratch
):
    mask, fwd_h, fwd_l, proj_h, proj_l, weights, sems = scratch
    columns = quarters(mask)
    masks = [pltpu.make_async_copy(mask_hbm, mask, sems.at[0, 0])]
    tables = [
        pltpu.make_async_copy(fwd_h_hbm, fwd_h, sems.at[1, 0]),
        pltpu.make_async_copy(fwd_l_hbm, fwd_l, sems.at[1, 1]),
    ]
    last = [
        pltpu.make_async_copy(weights_hbm, weights, sems.at[2, 2]),
        pltpu.make_async_copy(proj_h_hbm, proj_h, sems.at[2, 0]),
        pltpu.make_async_copy(proj_l_hbm, proj_l, sems.at[2, 1]),
    ]
    for copy in [*masks, *tables, *last]:
        copy.start()
    last[0].wait()
    kernels, width = share_out.shape
    whole = weights[0]
    for k in range(1, kernels):
        whole = whole + weights[k]
    rows = [jnp.full((1, width), weights[k], F32) for k in range(kernels)]
    share_out[...] = jnp.concatenate(rows, axis=0) / jnp.full((kernels, width), whole, F32)
    masks[0].wait()
    rows = []
    for cols in columns:
        transmit = jnp.tanh(mask[:, cols])
        slope_out[:, cols] = 1.0 - transmit * transmit
        rows.append(transmit)
    for copy in tables:
        copy.wait()
    terms = dot3(split(jnp.concatenate(rows, axis=0)), (fwd_h[...], fwd_l[...]))
    count = mask.shape[0]
    spectra = terms[:count]
    for i in range(1, QUARTERS):
        spectra = spectra + quarter_turn(terms[i * count : (i + 1) * count], -i)
    for copy in last[1:]:
        copy.wait()
    parts = dot3((proj_h[...], proj_l[...]), split(turn(spectra, -1)))
    half = parts.shape[0] // 2
    return parts[:half], parts[half:]


def project_first(*refs):
    args, (far, near, own, share, slope), scratch = refs[:6], refs[6:11], refs[11:]

    @pl.when(jnp.logical_not(is_last()))
    def _():
        low, high = project(*args, slope, share, scratch)
        odd = is_odd()
        far[...] = jnp.where(odd, high, low)
        near[...] = jnp.where(odd, low, high)
        own[...] = low + high


def project_second(*refs):
    args, taken, refs = refs[:6], refs[6:10], refs[11:]
    (far, near, own, share, slope), scratch = refs[:5], refs[5:]

    @pl.when(is_last())
    def _():
        low, high = project(*args, slope, share, scratch)
        far[...], near[...], own[...] = high, low, low + high

    @pl.when(jnp.logical_not(is_last()))
    def _():
        far[...], near[...], own[...], share[...] = (ref[...] for ref in taken)


def image(
    own, far, near, spectra, shares, target, rows_f, rows_t, cols_h, cols_l,
    wide_r, wide_rt, wide_h, wide_l, resist_hbm, grad_out, fields, resist_out, sem
):
    kernels, freq_rows, freq_cols = spectra.shape[1:]
    rows_c, cols_c = rows_f.shape[0] // 2, 2 * freq_cols
    group = math.gcd(kernels, GROUP)
    sign = alternate(own.shape)
    window = own[...] + sign * (far[...] + near[...])
    win_re, win_im = window[:, :freq_cols], window[:, freq_cols:]

    def forward(step, total):
        start = step * group
        prods = []
        for j in range(group):
            kern_re, kern_im = spectra[0, start + j], spectra[1, start + j]
            prods.append(jnp.concatenate(
                [kern_re * win_re - kern_im * win_im, kern_re * win_im + kern_im * win_re], axis=1
            ))
        inner = dot3(split(jnp.concatenate(prods, axis=0)), (cols_h[...], cols_l[...]))
        for j in range(group):
            part = inner[j * freq_rows : (j + 1) * freq_rows]
            part = jnp.concatenate([part[:, :cols_c], part[:, cols_c:]], axis=0)
            field = dot(rows_f[...], stack_right(part))
            fields[start + j] = field
            power = field[:rows_c] ** 2 + field[rows_c:] ** 2
            total = total + shares[pl.ds(start + j, 1), :] * power
        return total

    total = lax.fori_loop(0, kernels // group, forward, jnp.zeros((rows_c, cols_c), F32))
    tall = dot(wide_r[...], stack_right(total))
    intensity = dot3(split(tall), (wide_h[...], wide_l[...]))
    resist = jax.nn.sigmoid(STEEPNESS * (intensity - THRESHOLD))
    resist_out[...] = resist
    sent = pltpu.make_async_copy(resist_out, resist_hbm, sem)
    sent.start()
    slopes = (4.0 * STEEPNESS) * (resist - target[...].astype(F32)) * resist * (1.0 - resist)
    narrow = dot3_t(split(slopes), (wide_h[...], wide_l[...]))
    weight = dot(wide_rt[...], stack_right(narrow))
    weight = jnp.concatenate([weight, weight], axis=0)

    def backward(step, sums):
        grad_re, grad_im = sums
        start = step * group
        inners = []
        for j in range(group):
            pieces = jnp.concatenate(split(weight * fields[start + j]), axis=0)
            part = dot(rows_t[...], pieces)
            part = part[: 2 * freq_rows] + part[2 * freq_rows :]
            inners.append(jnp.concatenate([part[:freq_rows], part[freq_rows:]], axis=1))
        spec = dot3_t(split(jnp.concatenate(inners, axis=0)), (cols_h[...], cols_l[...]))
        for j in range(group):
            part = shares[pl.ds(start + j, 1), :] * spec[j * freq_rows : (j + 1) * freq_rows]
            real, imag = part[:, :freq_cols], part[:, freq_cols:]
            kern_re, kern_im = spectra[0, start + j], spectra[1, start + j]
            grad_re = grad_re + real * kern_re + imag * kern_im
            grad_im = grad_im + imag * kern_re - real * kern_im
        return grad_re, grad_im

    none = jnp.zeros((freq_rows, freq_cols), F32)
    grad_re, grad_im = lax.fori_loop(0, kernels // group, backward, (none, none))
    grad_out[...] = jnp.concatenate([grad_re, grad_im], axis=1)
    sent.wait()


def image_first(*refs):
    @pl.when(jnp.logical_not(is_first()))
    def _():
        image(*refs)


def image_second(*refs):
    args, (_, grad_in), refs = refs[:14], refs[14:16], refs[16:]

    @pl.when(is_first())
    def _():
        image(*args, *refs)

    @pl.when(jnp.logical_not(is_first()))
    def _():
        refs[1][...] = grad_in[...]


def gradient(own, before, after, slope, rows_b, fwd_h, fwd_l, out_hbm, out, sems):
    half = out.shape[0] // 2
    sign = alternate(own.shape)
    low = stack_turned(own[...] + sign * before)
    high = stack_turned(own[...] + sign * after)
    merged = jnp.concatenate([dot(rows_b[:half], low), dot(rows_b[half:], high)], axis=0)
    parts = [quarter_turn(merged, i) for i in range(QUARTERS)]
    pieces = split(jnp.concatenate(parts, axis=0))
    terms = dot3_t(pieces, (fwd_h[...], fwd_l[...]))
    rows = out.shape[0]
    for i, cols in enumerate(quarters(out)):
        out[:, cols] = slope[:, cols] * terms[i * rows : (i + 1) * rows]
    sent = pltpu.make_async_copy(out, out_hbm, sems.at[0])
    sent.start()
    sent.wait()


def gradient_first(own, before, after, *refs):
    @pl.when(is_first())
    def _():
        gradient(own, before[...], after[...], *refs)


def gradient_second(own, before_even, before_odd, after, slope, rows_b, fwd_h, fwd_l, _, *refs):
    @pl.when(jnp.logical_not(is_first()))
    def _():
        before = jnp.where(is_odd(), before_odd[...], before_even[...])
        gradient(own, before, after[...], slope, rows_b, fwd_h, fwd_l, *refs)


VMEM = pl.BlockSpec(memory_space=pltpu.VMEM)
HBM = pl.BlockSpec(memory_space=pltpu.HBM)


def call(kernel, outs, args, flops, scratch, out_specs, in_specs=None, aliases=None):
    shapes = [jax.ShapeDtypeStruct(shape, F32) for shape in outs]
    moved = sum(math.prod(a.shape) * a.dtype.itemsize for a in args)
    moved += sum(4 * math.prod(shape) for shape in outs)
    return pl.pallas_call(
        kernel,
        out_shape=shapes,
        in_specs=in_specs or [VMEM] * len(args),
        out_specs=out_specs,
        scratch_shapes=scratch,
        input_output_aliases=aliases or {},
        compiler_params=pltpu.CompilerParams(vmem_limit_bytes=LIMIT),
        cost_estimate=pl.CostEstimate(flops=flops, bytes_accessed=moved, transcendentals=0),
    )(*args)


def permute(value, pairs):
    return lax.ppermute(value, "tiles", pairs)


def shards(mask_params, target, kernel_spectra, kernel_weights):
    strip_rows, columns = mask_params.shape
    kernels, freq_rows, freq_cols = kernel_spectra.shape[1:]
    tables = jax.tree.map(
        jnp.asarray, make_tables(strip_rows, MARGIN, columns, freq_rows, freq_cols)
    )
    count = lax.axis_size("tiles")
    assert 2 * MARGIN == strip_rows and count % 2 == 0 and count >= 6
    near_pairs = [(i, i ^ 1) for i in range(count)]
    far_pairs = [(i, (i + 1 if i % 2 else i - 1) % count) for i in range(count)]
    last = count - 1
    ends = [(last, 0), (0, last - 1), (last - 1, last), (1, 2), (2, 3), (3, 1)]
    wrap1_pairs = ends + near_pairs[4 : last - 1]
    up_pairs = [(i, (i + 1) % count) for i in range(count)]
    down_pairs = [(j, i) for i, j in up_pairs]
    pair, full, wide = (freq_rows, 2 * freq_cols), (strip_rows, columns), (kernels, 2 * freq_cols)
    area = strip_rows * columns

    args = [mask_params, *tables["forward"], *tables["project"]]
    held = [pltpu.VMEM(a.shape, a.dtype) for a in args]
    held += [pltpu.SMEM((kernels,), F32), pltpu.SemaphoreType.DMA((3, QUARTERS))]
    args.append(kernel_weights)
    args = [pltpu.with_memory_space_constraint(a, pltpu.HBM) for a in args]
    work = 60 * area * 2 * freq_cols
    send_far, send_near, own, share, slope = call(
        project_first, [pair, pair, pair, wide, full], args, work, held,
        in_specs=[HBM] * 6, out_specs=[VMEM] * 5,
    )
    far = permute(send_far, far_pairs)
    send_far, send_near, own, share, slope = call(
        project_second, [pair, pair, pair, wide, full],
        [*args, send_far, send_near, own, share, slope],
        work, held, in_specs=[HBM] * 6 + [VMEM] * 5, out_specs=[VMEM] * 5, aliases={10: 4},
    )
    near = permute(send_near, near_pairs)
    far_first = permute(send_far, wrap1_pairs)

    rows_c, cols_c = 2 * freq_rows, 2 * freq_cols
    held = [
        pltpu.VMEM((kernels, 2 * rows_c, cols_c), F32),
        pltpu.VMEM(full, F32),
        pltpu.SemaphoreType.DMA,
    ]
    rest = [
        kernel_spectra, share, target,
        tables["field_rows"], tables["field_rows_t"], *tables["field_cols"],
        tables["widen_rows"], tables["widen_rows_t"], *tables["widen_cols"],
    ]
    specs = [VMEM] * 14
    work = 24 * kernels * rows_c * cols_c * cols_c
    resist, grad = call(
        image_first, [full, pair], [own, far, near, *rest], work, held,
        in_specs=specs, out_specs=[HBM, VMEM],
    )
    grad_after_first = permute(grad, near_pairs)
    grad_before_even = permute(grad, up_pairs)
    resist, grad = call(
        image_second, [full, pair], [own, far_first, near, *rest, resist, grad], work, held,
        in_specs=specs + [HBM, VMEM], out_specs=[HBM, VMEM], aliases={14: 0},
    )
    grad_after = permute(grad, down_pairs)
    grad_before_odd = permute(grad, near_pairs)
    rest = [slope, tables["back_rows"], *tables["forward"]]
    held = [pltpu.VMEM(full, F32), pltpu.SemaphoreType.DMA((QUARTERS,))]
    work = 6 * area * 2 * freq_cols
    (gradient,) = call(
        gradient_first, [full], [grad, grad_before_even, grad_after_first, *rest], work, held,
        out_specs=[HBM],
    )
    (gradient,) = call(
        gradient_second, [full],
        [grad, grad_before_even, grad_before_odd, grad_after, *rest, gradient], work, held,
        in_specs=[VMEM] * 8 + [HBM], out_specs=[HBM], aliases={8: 0},
    )
    return (resist, gradient)


def solution(mesh):
    in_specs = (P(("parts", "tiles"), None), P(("parts", "tiles"), None), P(), P())
    out_specs = (P(("parts", "tiles"), None), P(("parts", "tiles"), None))
    return jax.shard_map(shards, mesh=mesh, in_specs=in_specs, out_specs=out_specs, check_vma=False)
```
